32 devices in a mesh: batch: 4 (over x, core), seq: 8 (over z, y).
Axes of the slice: x: 2, y: 2, z: 4, core: 2. Of those that a mesh axis runs over, the one named last changes fastest.
Arguments:
- layer_inputs: bfloat16 [25600, 800], P(('batch', 'seq')), may hold values from -24 to 24
- output_grads: bfloat16 [25600, 800], P(('batch', 'seq')), may hold values from -48 to 48
- input_inverse: float32 [800, 200], replicated, may hold values from -1 to 3
- output_inverse: float32 [800, 200], replicated, may hold values from -1 to 3
Outputs:
- input_factor: float32 [800, 200], P('seq')
- output_factor: float32 [800, 200], P('seq')
- preconditioned: bfloat16 [800, 800], replicated
The draws below stay inside these ranges and needn't reach their ends.
All inputs are finite; a program needn't handle non-finite values.
Results may differ from the reference program's by a relative error of at most 0.0075.
Values may be sent and summed in bfloat16 or wider, within the bound.
No kernel may reach another device: no remote copies, remote signals or barrier semaphores. Data moves between devices by JAX's collectives and lax.ppermute only.
A program may use at most 64 MiB of HBM per device.

```python
import math
import jax
import jax.numpy as jnp
from jax import lax

DIN = 800
DOUT = 800
BLOCK = 200
TOK_DEV = 800
TOKENS = 25600


def shared_latent(key):
    return jax.random.normal(jax.random.fold_in(key, 11), (TOKENS, BLOCK), jnp.float32)


def mixed_draw(key, width, salt, strength, limit):
    latent = shared_latent(key)
    mixing = jax.random.normal(jax.random.fold_in(key, salt), (BLOCK, width), jnp.float32) * (strength / math.sqrt(BLOCK))
    noise_key = jax.random.fold_in(key, salt + 1)
    noise = jax.random.normal(noise_key, (TOKENS, width), jnp.float32)
    row_ids = jnp.arange(TOKENS, dtype=jnp.int32)
    device = row_ids // TOK_DEV
    rising = 1.0 + 2.0 * row_ids.astype(jnp.float32) / TOKENS
    offset = jax.random.randint(jax.random.fold_in(key, salt + 3), (), 0, 32, jnp.int32)
    group = jnp.arange(width, dtype=jnp.int32) // (width // 32)
    spiked = (device[:, None] + offset) % 32 == group[None, :]
    boost = jnp.where(spiked, 3.0, 1.0)
    values = 0.6 * noise * rising[:, None] * boost + jnp.dot(latent, mixing)
    return jnp.clip(values, -limit, limit)


def draw_layer_inputs(key, part):
    return mixed_draw(key, DIN, 101, 1.0, 24.0).astype(jnp.bfloat16)


def draw_output_grads(key, part):
    return mixed_draw(key, DOUT, 201, 3.0, 48.0).astype(jnp.bfloat16)


def inverse_blocks(key, width):
    count = width // BLOCK
    noise_key = jax.random.fold_in(key, 301)
    noise = jax.random.normal(noise_key, (count, BLOCK, BLOCK), jnp.float32)
    symmetric = (noise + jnp.swapaxes(noise, 1, 2)) * (0.4 / math.sqrt(2.0 * BLOCK))
    diagonal = jnp.exp(jax.random.uniform(jax.random.fold_in(key, 302), (count, BLOCK), jnp.float32, math.log(0.5), math.log(2.0)))
    matrix = symmetric + jnp.eye(BLOCK, dtype=jnp.float32)[None, :, :] * diagonal[:, :, None]
    return jnp.clip(matrix, -1.0, 3.0).reshape(width, BLOCK)


def draw_input_inverse(key, part):
    return inverse_blocks(jax.random.fold_in(key, 401), DIN)


def draw_output_inverse(key, part):
    return inverse_blocks(jax.random.fold_in(key, 402), DOUT)


def setup_inputs(seed: int = 0) -> dict:
    key_of = jax.random.split(jax.random.key(seed), 5)
    return {
        "layer_inputs": draw_layer_inputs(jax.random.fold_in(key_of[4], 71), 0),
        "output_grads": draw_output_grads(jax.random.fold_in(key_of[4], 71), 0),
        "input_inverse": draw_input_inverse(jax.random.fold_in(key_of[4], 71), 0),
        "output_inverse": draw_output_inverse(jax.random.fold_in(key_of[4], 71), 0),
    }


def block_covariance(values):
    width = values.shape[1]
    products = []
    for number in range(width // BLOCK):
        columns = values[:, number * BLOCK:(number + 1) * BLOCK]
        products.append(jnp.dot(columns.T, columns, preferred_element_type=jnp.float32))
    return jnp.concatenate(products, axis=0)


def reference(layer_inputs, output_grads, input_inverse, output_inverse):
    inverse_count = 1.0 / TOKENS
    input_factor = block_covariance(layer_inputs) * inverse_count
    output_factor = block_covariance(output_grads) * inverse_count
    gradient = jnp.dot(layer_inputs.T, output_grads, preferred_element_type=jnp.float32) * inverse_count
    in_blocks = DIN // BLOCK
    out_blocks = DOUT // BLOCK
    right_side = jnp.einsum("imk,mkl->iml", gradient.reshape(DIN, out_blocks, BLOCK),
                            output_inverse.reshape(out_blocks, BLOCK, BLOCK),
                            precision=lax.Precision.HIGHEST).reshape(DIN, DOUT)
    applied = jnp.einsum("nij,njo->nio", input_inverse.reshape(in_blocks, BLOCK, BLOCK),
                         right_side.reshape(in_blocks, BLOCK, DOUT),
                         precision=lax.Precision.HIGHEST).reshape(DIN, DOUT)
    return input_factor, output_factor, applied.astype(jnp.bfloat16)
```

```python
import jax
import jax.numpy as jnp
from jax import lax
from jax.experimental import pallas as pl
from jax.experimental.pallas import tpu as pltpu
from jax.sharding import PartitionSpec as P

AXES = ("batch", "seq")
LANES = 128
PACK = 16
F32 = jnp.float32
BF16 = jnp.bfloat16
NN = (((1,), (0,)), ((), ()))
NT = (((1,), (1,)), ((), ()))
TN = (((0,), (0,)), ((), ()))


def dot(a, b, dims):
    return lax.dot_general(a, b, dims, preferred_element_type=F32)


def up(value, step):
    return -(-value // step) * step


class Plan:
    def __init__(self, tokens, width, block, nb, ns):
        self.tokens, self.width, self.block = tokens, width, block
        self.nb, self.ns = nb, ns
        self.blocks = width // block
        assert self.blocks == 4 and nb % 2 == 0 and nb >= 4 and ns >= 8
        self.half = up(block // 2, 8)
        self.full_tiles = width // LANES
        self.tail = width - self.full_tiles * LANES
        assert self.tail and LANES % self.tail == 0
        self.fold = LANES // self.tail
        self.fold_rows = up(-(-self.half // self.fold), 8)
        assert self.half * self.full_tiles % 8 == 0
        self.grad_rows = up(self.half * self.full_tiles + self.fold_rows, PACK)
        self.corner = block - LANES
        assert 0 < self.corner <= LANES and self.corner % 8 == 0
        self.cov_total = up(block + self.corner, PACK)
        units = self.cov_total // PACK
        self.quarter = -(-units // 4)
        self.cuts = [min(units, self.quarter + t * (units - self.quarter) // 3) for t in range(4)]
        self.cuts = [0] + self.cuts
        self.g = self.grad_rows // PACK
        self.c = max(self.cuts[t + 1] - self.cuts[t] for t in range(4))
        self.count = tokens * nb * ns
        self.owned = width // ns

    def slice_rows(self, q):
        start = (q // 2) * self.block + (q % 2) * self.half
        return start, (self.half if q % 2 == 0 else self.block - self.half)

    def pack_grad(self, rows):
        n = rows.shape[0]
        if n < self.half:
            rows = jnp.concatenate([rows, jnp.zeros((self.half - n, self.width), F32)], 0)
        parts = [rows[:, k * LANES:(k + 1) * LANES] for k in range(self.full_tiles)]
        last = rows[:, self.full_tiles * LANES:]
        short = self.fold * self.fold_rows - self.half
        if short:
            last = jnp.concatenate([last, jnp.zeros((short, self.tail), F32)], 0)
        parts.append(jnp.concatenate(
            [last[i * self.fold_rows:(i + 1) * self.fold_rows] for i in range(self.fold)], 1))
        stacked = jnp.concatenate(parts, 0)
        left = self.grad_rows - stacked.shape[0]
        if left:
            stacked = jnp.concatenate([stacked, jnp.zeros((left, LANES), F32)], 0)
        return stacked.reshape(self.g, PACK, LANES)

    def unpack_grad(self, packed):
        stacked = packed.reshape(self.grad_rows, LANES)
        parts = [stacked[k * self.half:(k + 1) * self.half] for k in range(self.full_tiles)]
        base = self.half * self.full_tiles
        folded = stacked[base:base + self.fold_rows]
        last = jnp.concatenate(
            [folded[:, i * self.tail:(i + 1) * self.tail] for i in range(self.fold)], 0)
        parts.append(last[:self.half])
        return jnp.concatenate(parts, 1)

    def pack_cov(self, matrix):
        corner = matrix[LANES:, LANES:]
        corner = jnp.concatenate([corner, jnp.zeros((self.corner, LANES - self.corner), F32)], 1)
        stacked = jnp.concatenate([matrix[:, :LANES], corner], 0)
        left = self.cov_total - stacked.shape[0]
        if left:
            stacked = jnp.concatenate([stacked, jnp.zeros((left, LANES), F32)], 0)
        return stacked.reshape(self.cov_total // PACK, PACK, LANES)


def place(plan):
    batch = lax.axis_index("batch")
    seq = lax.axis_index("seq")
    core = batch % 2
    xy = (batch // 2 % 2) * 2 + seq % 2
    owner_block = seq // (plan.ns // plan.blocks)
    return batch, seq, core, xy, owner_block


def partials_kernel(plan, x_ref, y_ref, p_ref, keep_ref, send_ref):
    _, _, core, xy, owner_block = place(plan)

    def put(owner_core, j, start, value):
        size = value.shape[0]

        @pl.when(core == owner_core)
        def _():
            keep_ref[j, pl.ds(start, size)] = value.astype(keep_ref.dtype)

        @pl.when(core != owner_core)
        def _():
            send_ref[j, pl.ds(start, size)] = value.astype(BF16)

    y = y_ref[...]
    for b in range(plan.blocks):
        lo, hi = b * plan.block, (b + 1) * plan.block
        xb = x_ref[:, lo:hi]
        pb = p_ref[lo:hi, :]
        p_high = pb.astype(BF16)
        p_low = (pb - p_high.astype(F32)).astype(BF16)
        xt = (dot(p_high, xb, NT) + dot(p_low, xb, NT)).astype(BF16)
        gb = dot(xt, y, NN)
        for h in range(2):
            q = 2 * b + h
            start, n = plan.slice_rows(q)
            rows = gb[start - lo:start - lo + n]
            put(q // 4, (q % 4) ^ xy, 0, plan.pack_grad(rows))
        for factor, ref in ((0, x_ref), (1, y_ref)):
            vb = ref[:, lo:hi]
            stacked = plan.pack_cov(dot(vb, vb, TN))
            slot = plan.g + (b ^ owner_block) * plan.c
            for t in range(4):
                piece = stacked[plan.cuts[t]:plan.cuts[t + 1]]
                put(factor, t ^ xy, slot, piece)


def split_kernel(plan, keep_ref, recv_ref, own_ref, *send_refs):
    own_ref[...] = keep_ref[0] + recv_ref[0].astype(F32)
    for j in range(1, 4):
        send_refs[j - 1][...] = (keep_ref[j] + recv_ref[j].astype(F32)).astype(BF16)


def sum_kernel(*refs):
    total = refs[0][...].astype(F32)
    for ref in refs[1:-1]:
        total = total + ref[...].astype(F32)
    refs[-1][...] = total.astype(refs[-1].dtype)


def first_pair_kernel(plan, *refs):
    parts, send_ref, cov_ref = refs[:-2], refs[-2], refs[-1]
    g, c = plan.g, plan.c

    def total(start, size):
        value = parts[0][pl.ds(start, size)].astype(F32)
        for ref in parts[1:]:
            value = value + ref[pl.ds(start, size)].astype(F32)
        return value

    send_ref[pl.ds(0, g)] = total(0, g).astype(BF16)
    send_ref[pl.ds(g, c)] = total(g + c, c).astype(BF16)
    send_ref[pl.ds(g + c, c)] = total(g + 3 * c, c).astype(BF16)
    cov_ref[pl.ds(0, c)] = total(g, c)
    cov_ref[pl.ds(c, c)] = total(g + 2 * c, c)


def second_pair_kernel(plan, mine_ref, recv_ref, cov_ref, send_ref, keep_ref):
    g, c = plan.g, plan.c
    grad = mine_ref[pl.ds(0, g)].astype(F32) + recv_ref[pl.ds(0, g)].astype(F32)
    send_ref[pl.ds(0, g)] = grad.astype(BF16)
    other = cov_ref[pl.ds(c, c)] + recv_ref[pl.ds(g + c, c)].astype(F32)
    send_ref[pl.ds(g, c)] = other.astype(BF16)
    keep_ref[...] = cov_ref[pl.ds(0, c)] + recv_ref[pl.ds(g, c)].astype(F32)


def finish_kernel(plan, mine_ref, recv_ref, cov_ref, q_ref, out_ref):
    g, c, block = plan.g, plan.c, plan.block
    grad = mine_ref[pl.ds(0, g)].astype(F32) + recv_ref[pl.ds(0, g)].astype(F32)
    rows = plan.unpack_grad(grad) * (1.0 / plan.count)
    done = []
    for b in range(plan.blocks):
        part = rows[:, b * block:(b + 1) * block]
        high = part.astype(BF16)
        low = (part - high.astype(F32)).astype(BF16)
        qb = q_ref[b * block:(b + 1) * block, :]
        q_high = qb.astype(BF16)
        q_low = (qb - q_high.astype(F32)).astype(BF16)
        done.append(dot(high, q_high, NN) + (dot(high, q_low, NN) + dot(low, q_high, NN)))
    out_ref[pl.ds(0, g)] = plan.pack_grad(jnp.concatenate(done, 1)).astype(BF16)
    out_ref[pl.ds(g, c)] = (cov_ref[...] + recv_ref[pl.ds(g, c)].astype(F32)).astype(BF16)


def assemble_kernel(plan, *refs):
    bundles, (in_ref, out_ref, grad_ref, whole, sems) = refs[:8], refs[8:]
    _, seq, core, xy, _ = place(plan)
    g, block = plan.g, plan.block
    copies = []
    for i in range(8):
        q = (core ^ (i // 4)) * 4 + (xy ^ (i % 4))
        copy = pltpu.make_async_copy(bundles[i], whole.at[q], sems.at[i])
        copy.start()
        copies.append(copy)
    for copy in copies:
        copy.wait()
    for pair in range(plan.blocks // 2):
        rows = []
        for q in range(4 * pair, 4 * pair + 4):
            n = plan.slice_rows(q)[1]
            rows.append(plan.unpack_grad(whole[q, pl.ds(0, g)].astype(F32))[:n])
        grad_ref[pl.ds(2 * pair * block, 2 * block), :] = jnp.concatenate(rows, 0).astype(BF16)
    first = (seq % (plan.ns // plan.blocks)) * plan.owned
    row = lax.broadcasted_iota(jnp.int32, (plan.owned, block), 0) + first
    column = lax.broadcasted_iota(jnp.int32, (plan.owned, block), 1)
    select = jnp.where(row == column, 1.0, 0.0).astype(BF16)
    r128 = lax.broadcasted_iota(jnp.int32, (LANES, LANES), 0)
    c128 = lax.broadcasted_iota(jnp.int32, (LANES, LANES), 1)
    eye = jnp.where(r128 == c128, 1.0, 0.0).astype(BF16)
    for factor, ref in ((0, in_ref), (1, out_ref)):
        pieces = [
            whole[factor * 4 + t, pl.ds(g, plan.cuts[t + 1] - plan.cuts[t])].astype(F32)
            for t in range(4)
        ]
        stacked = jnp.concatenate(pieces, 0).reshape(plan.cov_total, LANES)
        left = stacked[:block]
        corner = stacked[block:block + plan.corner, :plan.corner]
        top = dot(eye, left[LANES:].astype(BF16), NT)
        right = jnp.concatenate([top, corner], 0)
        both = jnp.concatenate([left, right], 1).astype(BF16)
        ref[...] = dot(select, both, NN) * (1.0 / plan.count)


def call(kernel, shapes, args, scratch=(), name=None):
    vmem = pl.BlockSpec(memory_space=pltpu.VMEM)
    return pl.pallas_call(
        kernel,
        out_shape=[jax.ShapeDtypeStruct(s, d) for s, d in shapes],
        in_specs=[vmem] * len(args),
        out_specs=[vmem] * len(shapes),
        scratch_shapes=list(scratch),
        name=name,
    )(*args)


def solution(mesh):
    nb, ns = mesh.shape["batch"], mesh.shape["seq"]

    def swap(value, batch_bits, seq_bits):
        pairs = [
            (b * ns + s, (b ^ batch_bits) * ns + (s ^ seq_bits))
            for b in range(nb) for s in range(ns)
        ]
        return lax.ppermute(value, AXES, pairs)

    def shards(layer_inputs, output_grads, input_inverse, output_inverse):
        tokens, width = layer_inputs.shape
        plan = Plan(tokens, width, input_inverse.shape[1], nb, ns)
        g, c = plan.g, plan.c

        def bind(kernel):
            def bound(*refs):
                return kernel(plan, *refs)
            return bound

        full, tile = g + 4 * c, (PACK, LANES)
        keep, send = call(
            bind(partials_kernel), [((4, full, *tile), F32), ((4, full, *tile), BF16)],
            (layer_inputs, output_grads, input_inverse), name="partials")
        recv = swap(send, 1, 0)
        own, *sends = call(
            bind(split_kernel), [((full, *tile), F32)] + [((full, *tile), BF16)] * 3,
            (keep, recv), name="split")
        diagonal = swap(sends[2], 2, 1)
        parts = [own, swap(sends[0], 0, 1), swap(sends[1], 2, 0), diagonal]
        step = ns // plan.blocks
        extra = [(bit, 0) for bit in (4, 8, 16, 32, 64) if bit < nb]
        extra += [(0, bit) for bit in (2, 4, 8, 16, 32, 64) if bit < step]
        for batch_bit, seq_bit in extra:
            total, = call(sum_kernel, [((full, *tile), BF16)], parts, name="sum")
            parts = [total, swap(total, batch_bit, seq_bit)]
        mine, cov = call(
            bind(first_pair_kernel), [((g + 2 * c, *tile), BF16), ((2 * c, *tile), F32)],
            parts, name="first_pair")
        recv = swap(mine, 0, step)
        mine, cov = call(
            bind(second_pair_kernel), [((g + c, *tile), BF16), ((c, *tile), F32)],
            (mine, recv, cov), name="second_pair")
        recv = swap(mine, 0, 2 * step)
        done, = call(
            bind(finish_kernel), [((g + c, *tile), BF16)],
            (mine, recv, cov, output_inverse), name="finish")
        diagonal = swap(done, 2, 1)
        mine = [done, swap(done, 0, 1), swap(done, 2, 0), diagonal]
        theirs = [swap(value, 1, 0) for value in mine]
        in_factor, out_factor, grad = call(
            bind(assemble_kernel),
            [((plan.owned, plan.block), F32)] * 2 + [((width, width), BF16)],
            mine + theirs,
            scratch=[pltpu.VMEM((8, g + c, *tile), BF16), pltpu.SemaphoreType.DMA((8,))],
            name="assemble")
        return in_factor, out_factor, grad

    return jax.shard_map(
        shards,
        mesh=mesh,
        in_specs=(P(AXES, None), P(AXES, None), P(), P()),
        out_specs=(P("seq", None), P("seq", None), P()),
        check_vma=False,
    )
```

```python
import jax
import jax.numpy as jnp
from jax import lax
from jax.experimental import pallas as pl
from jax.experimental.pallas import tpu as pltpu
from jax.sharding import PartitionSpec as P

AXES = ("batch", "seq")
LANES = 128
PACK = 16
VMEM_LIMIT = 16 << 20
F32 = jnp.float32
BF16 = jnp.bfloat16
NN = (((1,), (0,)), ((), ()))
NT = (((1,), (1,)), ((), ()))
TN = (((0,), (0,)), ((), ()))


def dot(a, b, dims):
    return lax.dot_general(a, b, dims, preferred_element_type=F32)


def up(value, step):
    return -(-value // step) * step


class Plan:
    def __init__(self, tokens, width, block, nb, ns):
        self.tokens, self.width, self.block = tokens, width, block
        self.nb, self.ns = nb, ns
        self.blocks = width // block
        assert self.blocks == 4 and nb % 2 == 0 and nb >= 4 and ns >= 8
        self.half = up(block // 2, 8)
        self.full_tiles = width // LANES
        self.tail = width - self.full_tiles * LANES
        assert self.tail and LANES % self.tail == 0
        self.fold = LANES // self.tail
        self.fold_rows = up(-(-self.half // self.fold), 8)
        assert self.half * self.full_tiles % 8 == 0
        self.grad_rows = up(self.half * self.full_tiles + self.fold_rows, PACK)
        self.corner = block - LANES
        assert 0 < self.corner <= LANES and self.corner % 8 == 0
        self.cov_total = up(block + self.corner, PACK)
        units = self.cov_total // PACK
        self.quarter = -(-units // 4)
        self.cuts = [min(units, self.quarter + t * (units - self.quarter) // 3) for t in range(4)]
        self.cuts = [0] + self.cuts
        self.g = self.grad_rows // PACK
        self.c = max(self.cuts[t + 1] - self.cuts[t] for t in range(4))
        self.count = tokens * nb * ns
        self.owned = width // ns

    def slice_rows(self, q):
        start = (q // 2) * self.block + (q % 2) * self.half
        return start, (self.half if q % 2 == 0 else self.block - self.half)

    def pack_grad(self, rows):
        n = rows.shape[0]
        if n < self.half:
            rows = jnp.concatenate([rows, jnp.zeros((self.half - n, self.width), F32)], 0)
        parts = [rows[:, k * LANES:(k + 1) * LANES] for k in range(self.full_tiles)]
        last = rows[:, self.full_tiles * LANES:]
        short = self.fold * self.fold_rows - self.half
        if short:
            last = jnp.concatenate([last, jnp.zeros((short, self.tail), F32)], 0)
        parts.append(jnp.concatenate(
            [last[i * self.fold_rows:(i + 1) * self.fold_rows] for i in range(self.fold)], 1))
        stacked = jnp.concatenate(parts, 0)
        left = self.grad_rows - stacked.shape[0]
        if left:
            stacked = jnp.concatenate([stacked, jnp.zeros((left, LANES), F32)], 0)
        return stacked.reshape(self.g, PACK, LANES)

    def unpack_grad(self, packed):
        stacked = packed.reshape(self.grad_rows, LANES)
        parts = [stacked[k * self.half:(k + 1) * self.half] for k in range(self.full_tiles)]
        base = self.half * self.full_tiles
        folded = stacked[base:base + self.fold_rows]
        last = jnp.concatenate(
            [folded[:, i * self.tail:(i + 1) * self.tail] for i in range(self.fold)], 0)
        parts.append(last[:self.half])
        return jnp.concatenate(parts, 1)

    def pack_cov(self, matrix):
        corner = matrix[LANES:, LANES:]
        corner = jnp.concatenate([corner, jnp.zeros((self.corner, LANES - self.corner), F32)], 1)
        stacked = jnp.concatenate([matrix[:, :LANES], corner], 0)
        left = self.cov_total - stacked.shape[0]
        if left:
            stacked = jnp.concatenate([stacked, jnp.zeros((left, LANES), F32)], 0)
        return stacked.reshape(self.cov_total // PACK, PACK, LANES)


def place(plan):
    batch = lax.axis_index("batch")
    seq = lax.axis_index("seq")
    core = batch % 2
    xy = (batch // 2 % 2) * 2 + seq % 2
    owner_block = seq // (plan.ns // plan.blocks)
    return batch, seq, core, xy, owner_block


def partials_kernel(plan, x_ref, y_ref, p_ref, keep_ref, send_ref):
    _, _, core, xy, owner_block = place(plan)

    def put(owner_core, j, start, value):
        size = value.shape[0]

        @pl.when(core == owner_core)
        def _():
            keep_ref[j, pl.ds(start, size)] = value.astype(keep_ref.dtype)

        @pl.when(core != owner_core)
        def _():
            send_ref[j, pl.ds(start, size)] = value.astype(BF16)

    y = y_ref[...]
    for b in range(plan.blocks):
        lo, hi = b * plan.block, (b + 1) * plan.block
        xb = x_ref[:, lo:hi]
        pb = p_ref[:, lo:hi].T
        p_high = pb.astype(BF16)
        p_low = (pb - p_high.astype(F32)).astype(BF16)
        xt = (dot(p_high, xb, NT) + dot(p_low, xb, NT)).astype(BF16)
        gb = dot(xt, y, NN)
        for h in range(2):
            q = 2 * b + h
            start, n = plan.slice_rows(q)
            rows = gb[start - lo:start - lo + n]
            put(q // 4, (q % 4) ^ xy, 0, plan.pack_grad(rows))
        for factor, ref in ((0, x_ref), (1, y_ref)):
            vb = ref[:, lo:hi]
            stacked = plan.pack_cov(dot(vb, vb, TN))
            slot = plan.g + (b ^ owner_block) * plan.c
            for t in range(4):
                piece = stacked[plan.cuts[t]:plan.cuts[t + 1]]
                put(factor, t ^ xy, slot, piece)


def split_kernel(plan, keep_ref, recv_ref, own_ref, *send_refs):
    own_ref[...] = keep_ref[0] + recv_ref[0].astype(F32)
    for j in range(1, 4):
        send_refs[j - 1][...] = (keep_ref[j] + recv_ref[j].astype(F32)).astype(BF16)


def sum_kernel(*refs):
    total = refs[0][...].astype(F32)
    for ref in refs[1:-1]:
        total = total + ref[...].astype(F32)
    refs[-1][...] = total.astype(refs[-1].dtype)


def first_pair_kernel(plan, *refs):
    parts, send_ref, cov_ref = refs[:-2], refs[-2], refs[-1]
    g, c = plan.g, plan.c

    def total(start, size):
        value = parts[0][pl.ds(start, size)].astype(F32)
        for ref in parts[1:]:
            value = value + ref[pl.ds(start, size)].astype(F32)
        return value

    send_ref[pl.ds(0, g)] = total(0, g).astype(BF16)
    send_ref[pl.ds(g, c)] = total(g + c, c).astype(BF16)
    send_ref[pl.ds(g + c, c)] = total(g + 3 * c, c).astype(BF16)
    cov_ref[pl.ds(0, c)] = total(g, c)
    cov_ref[pl.ds(c, c)] = total(g + 2 * c, c)


def second_pair_kernel(plan, mine_ref, recv_ref, cov_ref, send_ref, keep_ref):
    g, c = plan.g, plan.c
    grad = mine_ref[pl.ds(0, g)].astype(F32) + recv_ref[pl.ds(0, g)].astype(F32)
    send_ref[pl.ds(0, g)] = grad.astype(BF16)
    other = cov_ref[pl.ds(c, c)] + recv_ref[pl.ds(g + c, c)].astype(F32)
    send_ref[pl.ds(g, c)] = other.astype(BF16)
    keep_ref[...] = cov_ref[pl.ds(0, c)] + recv_ref[pl.ds(g, c)].astype(F32)


def finish_kernel(plan, mine_ref, recv_ref, cov_ref, q_ref, out_ref):
    g, c, block = plan.g, plan.c, plan.block
    grad = mine_ref[pl.ds(0, g)].astype(F32) + recv_ref[pl.ds(0, g)].astype(F32)
    rows = plan.unpack_grad(grad) * (1.0 / plan.count)
    done = []
    for b in range(plan.blocks):
        part = rows[:, b * block:(b + 1) * block]
        high = part.astype(BF16)
        low = (part - high.astype(F32)).astype(BF16)
        qb = q_ref[:, b * block:(b + 1) * block]
        q_high = qb.astype(BF16)
        q_low = (qb - q_high.astype(F32)).astype(BF16)
        done.append(dot(high, q_high, NT) + (dot(high, q_low, NT) + dot(low, q_high, NT)))
    out_ref[pl.ds(0, g)] = plan.pack_grad(jnp.concatenate(done, 1)).astype(BF16)
    out_ref[pl.ds(g, c)] = (cov_ref[...] + recv_ref[pl.ds(g, c)].astype(F32)).astype(BF16)


def assemble_kernel(plan, *refs):
    bundles, (in_ref, out_ref, grad_ref, whole, sems) = refs[:8], refs[8:]
    _, seq, core, xy, _ = place(plan)
    g, block = plan.g, plan.block
    copies = []
    for i in range(8):
        q = (core ^ (i // 4)) * 4 + (xy ^ (i % 4))
        copy = pltpu.make_async_copy(bundles[i], whole.at[q], sems.at[i])
        copy.start()
        copies.append(copy)
    for copy in copies:
        copy.wait()
    for pair in range(plan.blocks // 2):
        rows = []
        for q in range(4 * pair, 4 * pair + 4):
            n = plan.slice_rows(q)[1]
            rows.append(plan.unpack_grad(whole[q, pl.ds(0, g)].astype(F32))[:n])
        grad_ref[pl.ds(2 * pair * block, 2 * block), :] = jnp.concatenate(rows, 0).astype(BF16)
    first = (seq % (plan.ns // plan.blocks)) * plan.owned
    row = lax.broadcasted_iota(jnp.int32, (plan.owned, block), 0) + first
    column = lax.broadcasted_iota(jnp.int32, (plan.owned, block), 1)
    select = jnp.where(row == column, 1.0, 0.0).astype(BF16)
    r128 = lax.broadcasted_iota(jnp.int32, (LANES, LANES), 0)
    c128 = lax.broadcasted_iota(jnp.int32, (LANES, LANES), 1)
    eye = jnp.where(r128 == c128, 1.0, 0.0).astype(BF16)
    for factor, ref in ((0, in_ref), (1, out_ref)):
        pieces = [
            whole[factor * 4 + t, pl.ds(g, plan.cuts[t + 1] - plan.cuts[t])].astype(F32)
            for t in range(4)
        ]
        stacked = jnp.concatenate(pieces, 0).reshape(plan.cov_total, LANES)
        left = stacked[:block]
        corner = stacked[block:block + plan.corner, :plan.corner]
        top = dot(eye, left[LANES:].astype(BF16), NT)
        right = jnp.concatenate([top, corner], 0)
        both = jnp.concatenate([left, right], 1).astype(BF16)
        ref[...] = dot(both, select, NT) * (1.0 / plan.count)


def call(kernel, shapes, args, scratch=(), name=None):
    vmem = pl.BlockSpec(memory_space=pltpu.VMEM)
    return pl.pallas_call(
        kernel,
        out_shape=[jax.ShapeDtypeStruct(s, d) for s, d in shapes],
        in_specs=[vmem] * len(args),
        out_specs=[vmem] * len(shapes),
        scratch_shapes=list(scratch),
        compiler_params=pltpu.CompilerParams(vmem_limit_bytes=VMEM_LIMIT),
        name=name,
    )(*args)


def solution(mesh):
    nb, ns = mesh.shape["batch"], mesh.shape["seq"]

    def swap(value, batch_bits, seq_bits):
        pairs = [
            (b * ns + s, (b ^ batch_bits) * ns + (s ^ seq_bits))
            for b in range(nb) for s in range(ns)
        ]
        return lax.ppermute(value, AXES, pairs)

    def shards(layer_inputs, output_grads, input_inverse, output_inverse):
        tokens, width = layer_inputs.shape
        plan = Plan(tokens, width, input_inverse.shape[1], nb, ns)
        g, c = plan.g, plan.c

        def bind(kernel):
            def bound(*refs):
                return kernel(plan, *refs)
            return bound

        full, tile = g + 4 * c, (PACK, LANES)
        keep, send = call(
            bind(partials_kernel), [((4, full, *tile), F32), ((4, full, *tile), BF16)],
            (layer_inputs, output_grads, input_inverse.T), name="partials")
        recv = swap(send, 1, 0)
        own, *sends = call(
            bind(split_kernel), [((full, *tile), F32)] + [((full, *tile), BF16)] * 3,
            (keep, recv), name="split")
        diagonal = swap(sends[2], 2, 1)
        parts = [own, swap(sends[0], 0, 1), swap(sends[1], 2, 0), diagonal]
        step = ns // plan.blocks
        extra = [(bit, 0) for bit in (4, 8, 16, 32, 64) if bit < nb]
        extra += [(0, bit) for bit in (2, 4, 8, 16, 32, 64) if bit < step]
        for batch_bit, seq_bit in extra:
            total, = call(sum_kernel, [((full, *tile), BF16)], parts, name="sum")
            parts = [total, swap(total, batch_bit, seq_bit)]
        mine, cov = call(
            bind(first_pair_kernel), [((g + 2 * c, *tile), BF16), ((2 * c, *tile), F32)],
            parts, name="first_pair")
        recv = swap(mine, 0, step)
        mine, cov = call(
            bind(second_pair_kernel), [((g + c, *tile), BF16), ((c, *tile), F32)],
            (mine, recv, cov), name="second_pair")
        recv = swap(mine, 0, 2 * step)
        done, = call(
            bind(finish_kernel), [((g + c, *tile), BF16)],
            (mine, recv, cov, output_inverse.T), name="finish")
        diagonal = swap(done, 2, 1)
        mine = [done, swap(done, 0, 1), swap(done, 2, 0), diagonal]
        theirs = [swap(value, 1, 0) for value in mine]
        in_factor, out_factor, grad = call(
            bind(assemble_kernel),
            [((plan.block, plan.owned), F32)] * 2 + [((width, width), BF16)],
            mine + theirs,
            scratch=[pltpu.VMEM((8, g + c, *tile), BF16), pltpu.SemaphoreType.DMA((8,))],
            name="assemble")
        return in_factor.T, out_factor.T, grad

    return jax.shard_map(
        shards,
        mesh=mesh,
        in_specs=(P(AXES, None), P(AXES, None), P(), P()),
        out_specs=(P("seq", None), P("seq", None), P()),
        check_vma=False,
    )
```

```python
import jax
import jax.numpy as jnp
from jax import lax
from jax.experimental import pallas as pl
from jax.experimental.pallas import tpu as pltpu
from jax.sharding import PartitionSpec as P

AXES = ("batch", "seq")
LANES = 128
PACK = 16
VMEM_LIMIT = 16 << 20
F32 = jnp.float32
BF16 = jnp.bfloat16
NN = (((1,), (0,)), ((), ()))
NT = (((1,), (1,)), ((), ()))
TN = (((0,), (0,)), ((), ()))


def dot(a, b, dims):
    return lax.dot_general(a, b, dims, preferred_element_type=F32)


def up(value, step):
    return -(-value // step) * step


class Plan:
    def __init__(self, tokens, width, block, nb, ns):
        self.tokens, self.width, self.block = tokens, width, block
        self.nb, self.ns = nb, ns
        self.blocks = width // block
        assert self.blocks == 4 and nb % 2 == 0 and nb >= 4 and ns >= 8
        self.cols = 2 * block
        self.full_tiles = self.cols // LANES
        self.tail = self.cols - self.full_tiles * LANES
        assert self.tail and LANES % self.tail == 0 and block % 8 == 0
        self.fold = LANES // self.tail
        self.fold_rows = up(-(-block // self.fold), 8)
        self.grad_rows = up(block * self.full_tiles + self.fold_rows, PACK)
        self.corner = block - LANES
        assert 0 < self.corner <= LANES and self.corner % 8 == 0
        self.cov_total = up(block + self.corner, PACK)
        units = self.cov_total // PACK
        self.quarter = -(-units // 4)
        self.cuts = [min(units, self.quarter + t * (units - self.quarter) // 3) for t in range(4)]
        self.cuts = [0] + self.cuts
        self.g = self.grad_rows // PACK
        self.c = max(self.cuts[t + 1] - self.cuts[t] for t in range(4))
        self.count = tokens * nb * ns
        self.owned = width // ns

    def pack_grad(self, part):
        parts = [part[:, k * LANES:(k + 1) * LANES] for k in range(self.full_tiles)]
        last = part[:, self.full_tiles * LANES:]
        short = self.fold * self.fold_rows - self.block
        if short:
            last = jnp.concatenate([last, jnp.zeros((short, self.tail), F32)], 0)
        parts.append(jnp.concatenate(
            [last[i * self.fold_rows:(i + 1) * self.fold_rows] for i in range(self.fold)], 1))
        stacked = jnp.concatenate(parts, 0)
        left = self.grad_rows - stacked.shape[0]
        if left:
            stacked = jnp.concatenate([stacked, jnp.zeros((left, LANES), F32)], 0)
        return stacked.reshape(self.g, PACK, LANES)

    def unpack_grad(self, packed):
        stacked = packed.reshape(self.grad_rows, LANES)
        parts = [stacked[k * self.block:(k + 1) * self.block] for k in range(self.full_tiles)]
        base = self.block * self.full_tiles
        folded = stacked[base:base + self.fold_rows]
        last = jnp.concatenate(
            [folded[:, i * self.tail:(i + 1) * self.tail] for i in range(self.fold)], 0)
        parts.append(last[:self.block])
        return jnp.concatenate(parts, 1)

    def pack_cov(self, matrix):
        corner = matrix[LANES:, LANES:]
        corner = jnp.concatenate([corner, jnp.zeros((self.corner, LANES - self.corner), F32)], 1)
        stacked = jnp.concatenate([matrix[:, :LANES], corner], 0)
        left = self.cov_total - stacked.shape[0]
        if left:
            stacked = jnp.concatenate([stacked, jnp.zeros((left, LANES), F32)], 0)
        return stacked.reshape(self.cov_total // PACK, PACK, LANES)


def place(plan):
    batch = lax.axis_index("batch")
    seq = lax.axis_index("seq")
    core = batch % 2
    xy = (batch // 2 % 2) * 2 + seq % 2
    owner_block = seq // (plan.ns // plan.blocks)
    return batch, seq, core, xy, owner_block


def putter(core, keep_ref, send_ref):
    def put(owner_core, j, start, value):
        size = value.shape[0]

        @pl.when(core == owner_core)
        def _():
            keep_ref[j, pl.ds(start, size)] = value.astype(keep_ref.dtype)

        @pl.when(core != owner_core)
        def _():
            send_ref[j, pl.ds(start, size)] = value.astype(BF16)

    return put


def grad_kernel(plan, x_ref, y_ref, keep_ref, send_ref):
    _, _, core, xy, _ = place(plan)
    put = putter(core, keep_ref, send_ref)
    grad = dot(x_ref[...], y_ref[...], TN)
    for q in range(8):
        rows = grad[q // 2 * plan.block:(q // 2 + 1) * plan.block]
        part = rows[:, q % 2 * plan.cols:(q % 2 + 1) * plan.cols]
        put(q // 4, (q % 4) ^ xy, 0, plan.pack_grad(part))


def cov_kernel(plan, x_ref, y_ref, after_ref, keep_ref, send_ref):
    _, _, core, xy, owner_block = place(plan)
    put = putter(core, keep_ref, send_ref)
    for b in range(plan.blocks):
        for factor, ref in ((0, x_ref), (1, y_ref)):
            part = ref[:, b * plan.block:(b + 1) * plan.block]
            stacked = plan.pack_cov(dot(part, part, TN))
            slot = (b ^ owner_block) * plan.c
            for t in range(4):
                put(factor, t ^ xy, slot, stacked[plan.cuts[t]:plan.cuts[t + 1]])


def split_kernel(keep_ref, recv_ref, after_ref, own_ref, *send_refs):
    own_ref[...] = keep_ref[0] + recv_ref[0].astype(F32)
    for j in range(1, 4):
        send_refs[j - 1][...] = (keep_ref[j] + recv_ref[j].astype(F32)).astype(BF16)


def first_kernel(*refs):
    sum_kernel(*refs[:4], refs[-1])


def second_kernel(mine_ref, recv_ref, after_ref, out_ref):
    sum_kernel(mine_ref, recv_ref, out_ref)


def sum_kernel(*refs):
    total = refs[0][...].astype(F32)
    for ref in refs[1:-1]:
        total = total + ref[...].astype(F32)
    refs[-1][...] = total.astype(refs[-1].dtype)


def cov_first_kernel(plan, *refs):
    parts, send_ref, keep_ref = refs[:-2], refs[-2], refs[-1]
    c = plan.c
    for slot in range(plan.blocks):
        total = parts[0][pl.ds(slot * c, c)].astype(F32)
        for ref in parts[1:]:
            total = total + ref[pl.ds(slot * c, c)].astype(F32)
        if slot % 2:
            send_ref[pl.ds(slot // 2 * c, c)] = total.astype(BF16)
        else:
            keep_ref[pl.ds(slot // 2 * c, c)] = total


def cov_second_kernel(plan, mine_ref, recv_ref, send_ref, keep_ref):
    c = plan.c
    send_ref[...] = (mine_ref[pl.ds(c, c)] + recv_ref[pl.ds(c, c)].astype(F32)).astype(BF16)
    keep_ref[...] = mine_ref[pl.ds(0, c)] + recv_ref[pl.ds(0, c)].astype(F32)


def split_two(value):
    high = value.astype(BF16)
    return high, (value - high.astype(F32)).astype(BF16)


def dot_split(a, b, dims):
    a_high, a_low = split_two(a)
    b_high, b_low = split_two(b)
    return dot(a_high, b_high, dims) + (dot(a_high, b_low, dims) + dot(a_low, b_high, dims))


def pick(ref, plan, wanted, choices):
    value = ref[:, choices[0] * plan.block:(choices[0] + 1) * plan.block]
    for n in choices[1:]:
        value = jnp.where(wanted == n, ref[:, n * plan.block:(n + 1) * plan.block], value)
    return value


def finish_kernel(plan, mine_ref, recv_ref, cov_ref, cov_recv_ref, p_ref, q_ref, out_ref):
    _, _, core, xy, _ = place(plan)
    g, c, block = plan.g, plan.c, plan.block
    out_ref[pl.ds(g, c)] = (cov_ref[...] + cov_recv_ref[...].astype(F32)).astype(BF16)
    rows = plan.unpack_grad(mine_ref[...].astype(F32) + recv_ref[...].astype(F32))
    rows = rows * (1.0 / plan.count)
    p_turned = pick(p_ref, plan, core * 2 + xy // 2, range(plan.blocks))
    left = dot_split(p_turned.T, rows, NN)
    done = []
    for h in range(2):
        q_turned = pick(q_ref, plan, xy % 2 * 2 + h, (h, 2 + h))
        done.append(dot_split(left[:, h * block:(h + 1) * block], q_turned, NT))
    out_ref[pl.ds(0, g)] = plan.pack_grad(jnp.concatenate(done, 1)).astype(BF16)


def assemble_kernel(plan, *refs):
    bundles, (in_ref, out_ref, grad_ref, whole, sems) = refs[:8], refs[8:]
    _, seq, core, xy, _ = place(plan)
    g, block = plan.g, plan.block
    copies = []
    for i in range(8):
        q = (core ^ (i // 4)) * 4 + (xy ^ (i % 4))
        copy = pltpu.make_async_copy(bundles[i], whole.at[q], sems.at[i])
        copy.start()
        copies.append(copy)
    for copy in copies:
        copy.wait()
    for pair in range(plan.blocks // 2):
        rows = []
        for b in (2 * pair, 2 * pair + 1):
            rows.append(jnp.concatenate(
                [plan.unpack_grad(whole[2 * b + h, pl.ds(0, g)].astype(F32)) for h in range(2)], 1))
        grad_ref[pl.ds(2 * pair * block, 2 * block), :] = jnp.concatenate(rows, 0).astype(BF16)
    first = (seq % (plan.ns // plan.blocks)) * plan.owned
    row = lax.broadcasted_iota(jnp.int32, (plan.owned, block), 0) + first
    column = lax.broadcasted_iota(jnp.int32, (plan.owned, block), 1)
    select = jnp.where(row == column, 1.0, 0.0).astype(BF16)
    r128 = lax.broadcasted_iota(jnp.int32, (LANES, LANES), 0)
    c128 = lax.broadcasted_iota(jnp.int32, (LANES, LANES), 1)
    eye = jnp.where(r128 == c128, 1.0, 0.0).astype(BF16)
    for factor, ref in ((0, in_ref), (1, out_ref)):
        pieces = [
            whole[factor * 4 + t, pl.ds(g, plan.cuts[t + 1] - plan.cuts[t])].astype(F32)
            for t in range(4)
        ]
        stacked = jnp.concatenate(pieces, 0).reshape(plan.cov_total, LANES)
        left = stacked[:block]
        corner = stacked[block:block + plan.corner, :plan.corner]
        top = dot(eye, left[LANES:].astype(BF16), NT)
        right = jnp.concatenate([top, corner], 0)
        both = jnp.concatenate([left, right], 1).astype(BF16)
        ref[...] = dot(both, select, NT) * (1.0 / plan.count)


def call(kernel, shapes, args, scratch=(), name=None):
    vmem = pl.BlockSpec(memory_space=pltpu.VMEM)
    return pl.pallas_call(
        kernel,
        out_shape=[jax.ShapeDtypeStruct(s, d) for s, d in shapes],
        in_specs=[vmem] * len(args),
        out_specs=[vmem] * len(shapes),
        scratch_shapes=list(scratch),
        compiler_params=pltpu.CompilerParams(vmem_limit_bytes=VMEM_LIMIT),
        name=name,
    )(*args)


def solution(mesh):
    nb, ns = mesh.shape["batch"], mesh.shape["seq"]

    def swap(value, batch_bits, seq_bits):
        pairs = [
            (b * ns + s, (b ^ batch_bits) * ns + (s ^ seq_bits))
            for b in range(nb) for s in range(ns)
        ]
        return lax.ppermute(value, AXES, pairs)

    def shards(layer_inputs, output_grads, input_inverse, output_inverse):
        tokens, width = layer_inputs.shape
        plan = Plan(tokens, width, input_inverse.shape[1], nb, ns)
        g, c = plan.g, plan.c
        step = ns // plan.blocks
        extra = [(bit, 0) for bit in (4, 8, 16, 32, 64) if bit < nb]
        extra += [(0, bit) for bit in (2, 4, 8, 16, 32, 64) if bit < step]

        def bind(kernel):
            def bound(*refs):
                return kernel(plan, *refs)
            return bound

        def units(n, dtype, *lead):
            return (*lead, n, PACK, LANES), dtype

        def gather_parts(keep, send, after, n, name):
            own, *sends = call(
                split_kernel, [units(n, F32)] + [units(n, BF16)] * 3,
                (keep, swap(send, 1, 0), after), name=name)
            return [own, swap(sends[0], 0, 1), swap(sends[1], 2, 0), swap(sends[2], 2, 1)]

        def widen(parts, n):
            for batch_bit, seq_bit in extra:
                total, = call(sum_kernel, [units(n, BF16)], parts, name="sum")
                parts = [total, swap(total, batch_bit, seq_bit)]
            return parts

        keep, send = call(
            bind(grad_kernel), [units(g, F32, 4), units(g, BF16, 4)],
            (layer_inputs, output_grads), name="grad")
        cov_keep, cov_send = call(
            bind(cov_kernel), [units(4 * c, F32, 4), units(4 * c, BF16, 4)],
            (layer_inputs, output_grads, keep), name="cov")
        parts = gather_parts(keep, send, cov_keep, g, "split")
        cov_parts = gather_parts(cov_keep, cov_send, parts[0], 4 * c, "cov_split")
        mine, = call(first_kernel, [units(g, BF16)], parts + [cov_parts[0]], name="first")
        for batch_bit, seq_bit in extra:
            mine, = call(
                sum_kernel, [units(g, BF16)], (mine, swap(mine, batch_bit, seq_bit)), name="sum")
        recv = swap(mine, 0, step)
        cov_send, cov = call(
            bind(cov_first_kernel), [units(2 * c, BF16), units(2 * c, F32)],
            widen(cov_parts, 4 * c), name="cov_first")
        mine, = call(second_kernel, [units(g, BF16)], (mine, recv, cov), name="second")
        recv = swap(mine, 0, 2 * step)
        cov_send, cov = call(
            bind(cov_second_kernel), [units(c, BF16), units(c, F32)],
            (cov, swap(cov_send, 0, step)), name="cov_second")
        cov_recv = swap(cov_send, 0, 2 * step)
        done, = call(
            bind(finish_kernel), [units(g + c, BF16)],
            (mine, recv, cov, cov_recv, input_inverse.T, output_inverse.T), name="finish")
        mine = [done, swap(done, 0, 1), swap(done, 2, 0), swap(done, 2, 1)]
        theirs = [swap(value, 1, 0) for value in mine]
        in_factor, out_factor, grad = call(
            bind(assemble_kernel),
            [((plan.block, plan.owned), F32)] * 2 + [((width, width), BF16)],
            mine + theirs,
            scratch=[pltpu.VMEM(units(g + c, BF16, 8)[0], BF16), pltpu.SemaphoreType.DMA((8,))],
            name="assemble")
        return in_factor.T, out_factor.T, grad

    return jax.shard_map(
        shards,
        mesh=mesh,
        in_specs=(P(AXES, None), P(AXES, None), P(), P()),
        out_specs=(P("seq", None), P("seq", None), P()),
        check_vma=False,
    )
```

```python
import jax
import jax.numpy as jnp
from jax import lax
from jax.experimental import pallas as pl
from jax.experimental.pallas import tpu as pltpu
from jax.sharding import PartitionSpec as P


AXES = ("batch", "seq")
LANES = 128
PACK = 16
VMEM_LIMIT = 16 << 20
F32 = jnp.float32
BF16 = jnp.bfloat16
NN = (((1,), (0,)), ((), ()))
NT = (((1,), (1,)), ((), ()))


def dot(a, b, dims):
    return lax.dot_general(a, b, dims, preferred_element_type=F32)


def up(value, step):
    return -(-value // step) * step


class Plan:
    def __init__(self, tokens, width, block, nb, ns):
        self.tokens, self.width, self.block = tokens, width, block
        self.nb, self.ns = nb, ns
        self.blocks = width // block
        assert self.blocks == 4 and nb % 2 == 0 and nb >= 4 and ns >= 8
        assert LANES < block <= 2 * LANES and block % 8 == 0
        self.corner = block - LANES
        self.folds = []
        base, column = block, LANES
        while column < block:
            lanes = 1
            while column + 2 * lanes <= block:
                lanes *= 2
            rows = up(-(-block * lanes // LANES), 8)
            self.folds.append((column, lanes, base, rows))
            base, column = base + rows, column + lanes
        self.grad_rows = up(base, PACK)
        self.cov_total = up(block + self.corner, PACK)
        units = self.cov_total // PACK
        self.quarter = -(-units // 4)
        self.cuts = [min(units, self.quarter + t * (units - self.quarter) // 3) for t in range(4)]
        self.cuts = [0] + self.cuts
        self.g = self.grad_rows // PACK
        self.c = max(self.cuts[t + 1] - self.cuts[t] for t in range(4))
        self.count = tokens * nb * ns
        self.owned = width // ns

    def pack_grad(self, part):
        parts = [part[:, :LANES]]
        for column, lanes, _, rows in self.folds:
            piece = part[:, column:column + lanes]
            groups = -(-self.block // rows)
            short = groups * rows - self.block
            if short:
                piece = jnp.concatenate([piece, jnp.zeros((short, lanes), F32)], 0)
            row = [piece[i * rows:(i + 1) * rows] for i in range(groups)]
            if groups * lanes < LANES:
                row.append(jnp.zeros((rows, LANES - groups * lanes), F32))
            parts.append(jnp.concatenate(row, 1))
        stacked = jnp.concatenate(parts, 0)
        left = self.grad_rows - stacked.shape[0]
        if left:
            stacked = jnp.concatenate([stacked, jnp.zeros((left, LANES), F32)], 0)
        return stacked.reshape(self.g, PACK, LANES)

    def unpack_grad(self, packed):
        stacked = packed.reshape(self.grad_rows, LANES)
        parts = [stacked[:self.block]]
        for _, lanes, base, rows in self.folds:
            folded = stacked[base:base + rows]
            groups = -(-self.block // rows)
            piece = jnp.concatenate(
                [folded[:, i * lanes:(i + 1) * lanes] for i in range(groups)], 0)
            parts.append(piece[:self.block])
        return jnp.concatenate(parts, 1)

    def pack_cov(self, matrix):
        corner = matrix[LANES:, LANES:]
        corner = jnp.concatenate([corner, jnp.zeros((self.corner, LANES - self.corner), F32)], 1)
        stacked = jnp.concatenate([matrix[:, :LANES], corner], 0)
        left = self.cov_total - stacked.shape[0]
        if left:
            stacked = jnp.concatenate([stacked, jnp.zeros((left, LANES), F32)], 0)
        return stacked.reshape(self.cov_total // PACK, PACK, LANES)


def place(plan):
    batch = lax.axis_index("batch")
    seq = lax.axis_index("seq")
    core = batch % 2
    xy = (batch // 2 % 2) * 2 + seq % 2
    owner_block = seq // (plan.ns // plan.blocks)
    return seq, core, xy, owner_block


def putter(core, keep_ref, send_ref):
    def put(owner_core, at, value):
        @pl.when(core == owner_core)
        def _():
            keep_ref[at] = value.astype(keep_ref.dtype)

        @pl.when(core != owner_core)
        def _():
            send_ref[at] = value.astype(BF16)

    return put


def grad_kernel(plan, x_ref, y_ref, keep_ref, send_ref, turned_ref, x_own, y_own, sems):
    _, core, xy, owner_block = place(plan)
    copies = [
        pltpu.make_async_copy(x_ref, x_own, sems.at[0]),
        pltpu.make_async_copy(y_ref, y_own, sems.at[1]),
    ]
    for copy in copies:
        copy.start()
    put = putter(core, keep_ref, send_ref)
    copies[0].wait()
    turned = x_own[...].T
    turned_ref[...] = turned
    copies[1].wait()
    for column in range(plan.blocks):
        part = y_own[:, column * plan.block:(column + 1) * plan.block]
        grad = dot(turned, part, NN)
        slot = column % 2 ^ owner_block % 2
        for b in range(plan.blocks):
            packed = plan.pack_grad(grad[b * plan.block:(b + 1) * plan.block])
            put(b // 2, ((b % 2 * 2 + column // 2) ^ xy, slot), packed)


def cov_kernel(plan, x_ref, y_ref, turned_ref, keep_ref, send_ref):
    _, core, xy, owner_block = place(plan)
    put = putter(core, keep_ref, send_ref)
    block = plan.block
    for factor, ref in ((0, x_ref), (1, y_ref)):
        turned = turned_ref[...] if factor == 0 else ref[...].T
        for b in range(plan.blocks):
            part = ref[:, b * block:(b + 1) * block]
            stacked = plan.pack_cov(dot(turned[b * block:(b + 1) * block], part, NN))
            slot = (b ^ owner_block) * plan.c
            for t in range(4):
                piece = stacked[plan.cuts[t]:plan.cuts[t + 1]]
                put(factor, (t ^ xy, pl.ds(slot, piece.shape[0])), piece)


def split_kernel(keep_ref, recv_ref, after_ref, own_ref, *send_refs):
    own_ref[...] = keep_ref[0] + recv_ref[0].astype(F32)
    for j in range(1, 4):
        send_refs[j - 1][...] = (keep_ref[j] + recv_ref[j].astype(F32)).astype(BF16)


def total(parts, at):
    value = parts[0][at].astype(F32)
    for ref in parts[1:]:
        value = value + ref[at].astype(F32)
    return value


def sum_kernel(*refs):
    refs[-1][...] = total(refs[:-1], ...).astype(refs[-1].dtype)


def first_kernel(parts, outs):
    send_ref, keep_ref = outs
    keep_ref[...] = total(parts[:-1], 0)
    send_ref[...] = total(parts[:-1], 1).astype(BF16)


def second_kernel(plan, parts, outs):
    mine_ref, recv_ref, *cov_refs = parts
    send_ref, cov_ref = outs
    g, c = plan.g, plan.c
    send_ref[pl.ds(0, g)] = (mine_ref[...] + recv_ref[...].astype(F32)).astype(BF16)
    cov_ref[...] = total(cov_refs, pl.ds(0, 2 * c))
    send_ref[pl.ds(g, 2 * c)] = total(cov_refs, pl.ds(2 * c, 2 * c)).astype(BF16)


def split_two(value):
    high = value.astype(BF16)
    return high, (value - high.astype(F32)).astype(BF16)


def dot_split(a, b, dims):
    a_high, a_low = split_two(a)
    b_high, b_low = split_two(b)
    return dot(a_high, b_high, dims) + (dot(a_high, b_low, dims) + dot(a_low, b_high, dims))


def pick(ref, plan, wanted):
    value = ref[:, :plan.block]
    for n in range(1, plan.blocks):
        value = jnp.where(wanted == n, ref[:, n * plan.block:(n + 1) * plan.block], value)
    return value


def finish_kernel(plan, mine_ref, recv_ref, cov_ref, p_ref, q_ref, out_ref, keep_ref):
    _, core, xy, owner_block = place(plan)
    g, c = plan.g, plan.c
    keep_ref[...] = cov_ref[pl.ds(0, c)] + recv_ref[pl.ds(g, c)].astype(F32)
    other = cov_ref[pl.ds(c, c)] + recv_ref[pl.ds(g + c, c)].astype(F32)
    out_ref[pl.ds(g, c)] = other.astype(BF16)
    grad = mine_ref[pl.ds(0, g)].astype(F32) + recv_ref[pl.ds(0, g)].astype(F32)
    grad = plan.unpack_grad(grad) * (1.0 / plan.count)
    p_turned = pick(p_ref, plan, core * 2 + xy // 2)
    q_turned = pick(q_ref, plan, xy % 2 * 2 + owner_block % 2)
    done = dot_split(dot_split(p_turned.T, grad, NN), q_turned, NT)
    out_ref[pl.ds(0, g)] = plan.pack_grad(done).astype(BF16)


def bundle_kernel(plan, mine_ref, recv_ref, cov_ref, out_ref):
    g, c = plan.g, plan.c
    out_ref[pl.ds(0, g)] = mine_ref[pl.ds(0, g)]
    out_ref[pl.ds(g, g)] = recv_ref[pl.ds(0, g)]
    out_ref[pl.ds(2 * g, c)] = (cov_ref[...] + recv_ref[pl.ds(g, c)].astype(F32)).astype(BF16)


def assemble_kernel(plan, *refs):
    bundles, (in_ref, out_ref, grad_ref, whole, covs, done, sems, out_sems) = refs[:8], refs[8:]
    seq, core, xy, owner_block = place(plan)
    g, c, block = plan.g, plan.c, plan.block
    copies = []
    for i in range(8):
        q = (core ^ (i // 4)) * 4 + (xy ^ (i % 4))
        for e in range(2):
            copies.append(pltpu.make_async_copy(
                bundles[i].at[pl.ds(e * g, g)], whole.at[q * 2 + (e ^ owner_block % 2)],
                sems.at[3 * i + e]))
        copies.append(pltpu.make_async_copy(
            bundles[i].at[pl.ds(2 * g, c)], covs.at[q], sems.at[3 * i + 2]))
    for copy in copies:
        copy.start()
    for copy in copies:
        copy.wait()
    writes = []
    for b in range(plan.blocks):
        row = [plan.unpack_grad(whole[4 * b + n].astype(F32)) for n in range(plan.blocks)]
        done[b] = jnp.concatenate(row, 1).astype(BF16)
        write = pltpu.make_async_copy(
            done.at[b], grad_ref.at[pl.ds(b * block, block)], out_sems.at[b])
        write.start()
        writes.append(write)
    first = (seq % (plan.ns // plan.blocks)) * plan.owned
    row = lax.broadcasted_iota(jnp.int32, (plan.owned, block), 0) + first
    column = lax.broadcasted_iota(jnp.int32, (plan.owned, block), 1)
    select = jnp.where(row == column, 1.0, 0.0).astype(BF16)
    r128 = lax.broadcasted_iota(jnp.int32, (LANES, LANES), 0)
    c128 = lax.broadcasted_iota(jnp.int32, (LANES, LANES), 1)
    eye = jnp.where(r128 == c128, 1.0, 0.0).astype(BF16)
    for factor, ref in ((0, in_ref), (1, out_ref)):
        pieces = [
            covs[factor * 4 + t, pl.ds(0, plan.cuts[t + 1] - plan.cuts[t])].astype(F32)
            for t in range(4)
        ]
        stacked = jnp.concatenate(pieces, 0).reshape(plan.cov_total, LANES)
        left = stacked[:block]
        corner = stacked[block:block + plan.corner, :plan.corner]
        top = dot(eye, left[LANES:].astype(BF16), NT)
        right = jnp.concatenate([top, corner], 0)
        both = jnp.concatenate([left, right], 1).astype(BF16)
        ref[...] = dot(both, select, NT) * (1.0 / plan.count)
    for write in writes:
        write.wait()


def call(kernel, shapes, args, scratch=(), hbm_in=0, hbm_out=()):
    vmem = pl.BlockSpec(memory_space=pltpu.VMEM)
    hbm = pl.BlockSpec(memory_space=pltpu.HBM)
    args = [
        pltpu.with_memory_space_constraint(a, pltpu.HBM) if i < hbm_in else a
        for i, a in enumerate(args)
    ]
    return pl.pallas_call(
        kernel,
        out_shape=[jax.ShapeDtypeStruct(s, d) for s, d in shapes],
        in_specs=[hbm if i < hbm_in else vmem for i in range(len(args))],
        out_specs=[hbm if i in hbm_out else vmem for i in range(len(shapes))],
        scratch_shapes=list(scratch),
        compiler_params=pltpu.CompilerParams(vmem_limit_bytes=VMEM_LIMIT),
    )(*args)


def solution(mesh):
    nb, ns = mesh.shape["batch"], mesh.shape["seq"]

    def swap(value, batch_bits, seq_bits):
        pairs = [
            (b * ns + s, (b ^ batch_bits) * ns + (s ^ seq_bits))
            for b in range(nb) for s in range(ns)
        ]
        return lax.ppermute(value, AXES, pairs)

    def shards(layer_inputs, output_grads, input_inverse, output_inverse):
        tokens, width = layer_inputs.shape
        plan = Plan(tokens, width, input_inverse.shape[1], nb, ns)
        g, c = plan.g, plan.c
        step = ns // plan.blocks
        extra = [(bit, 0) for bit in (4, 8, 16, 32, 64) if bit < nb]
        extra += [(0, bit) for bit in (2, 4, 8, 16, 32, 64) if bit < step]

        def bind(kernel):
            def bound(*refs):
                return kernel(plan, *refs)

            return bound

        def group(kernel, outs, *head):
            def bound(*refs):
                return kernel(*head, refs[:-outs], refs[-outs:])

            return bound

        def units(n, dtype, *lead):
            return (*lead, n, PACK, LANES), dtype

        def exchange_parts(keep, send, after, shape):
            own, *sends = call(
                split_kernel, [(shape, F32)] + [(shape, BF16)] * 3,
                (keep, swap(send, 1, 0), after))
            peers = [swap(sends[2], 2, 1), swap(sends[1], 2, 0), swap(sends[0], 0, 1)]
            return [own] + peers

        def widen(parts, shape):
            for batch_bit, seq_bit in extra:
                summed, = call(sum_kernel, [(shape, BF16)], parts)
                parts = [summed, swap(summed, batch_bit, seq_bit)]
            return parts

        tile = (PACK, LANES)
        keep, send, turned = call(
            bind(grad_kernel),
            [units(g, F32, 4, 2), units(g, BF16, 4, 2), ((width, tokens), BF16)],
            (layer_inputs, output_grads), hbm_in=2,
            scratch=[pltpu.VMEM((tokens, width), BF16)] * 2 + [pltpu.SemaphoreType.DMA((2,))])
        cov_keep, cov_send = call(
            bind(cov_kernel), [units(4 * c, F32, 4), units(4 * c, BF16, 4)],
            (layer_inputs, output_grads, turned))
        parts = exchange_parts(keep, send, cov_keep, (2, g, *tile))
        cov_parts = exchange_parts(cov_keep, cov_send, parts[0], (4 * c, *tile))
        send, keep = call(
            group(first_kernel, 2), [units(g, BF16), units(g, F32)],
            widen(parts, (2, g, *tile)) + [cov_parts[0]])
        send, cov = call(
            group(second_kernel, 2, plan), [units(g + 2 * c, BF16), units(2 * c, F32)],
            [keep, swap(send, 0, step)] + widen(cov_parts, (4 * c, *tile)))
        send, cov = call(
            bind(finish_kernel), [units(g + c, BF16), units(c, F32)],
            (send, swap(send, 0, 2 * step), cov, input_inverse.T, output_inverse.T))
        done, = call(
            bind(bundle_kernel), [units(2 * g + c, BF16)],
            (send, swap(send, 0, step), cov))
        mine = [done, swap(done, 0, 1), swap(done, 2, 0), swap(done, 2, 1)]
        theirs = [swap(value, 1, 0) for value in mine]
        in_factor, out_factor, grad = call(
            bind(assemble_kernel),
            [((plan.block, plan.owned), F32)] * 2 + [((width, width), BF16)],
            mine + theirs, hbm_out=(2,),
            scratch=[
                pltpu.VMEM(units(g, BF16, 16)[0], BF16), pltpu.VMEM(units(c, BF16, 8)[0], BF16),
                pltpu.VMEM((plan.blocks, plan.block, width), BF16),
                pltpu.SemaphoreType.DMA((24,)), pltpu.SemaphoreType.DMA((plan.blocks,))])
        return in_factor.T, out_factor.T, grad

    return jax.shard_map(
        shards,
        mesh=mesh,
        in_specs=(P(AXES, None), P(AXES, None), P(), P()),
        out_specs=(P("seq", None), P("seq", None), P()),
        check_vma=False,
    )
```

```python
import jax
import jax.numpy as jnp
from jax import lax
from jax.experimental import pallas as pl
from jax.experimental.pallas import tpu as pltpu
from jax.sharding import PartitionSpec as P


AXES = ("batch", "seq")
LANES = 128
PACK = 16
VMEM_LIMIT = 16 << 20
F32 = jnp.float32
BF16 = jnp.bfloat16
NN = (((1,), (0,)), ((), ()))
NT = (((1,), (1,)), ((), ()))
TN = (((0,), (0,)), ((), ()))


def dot(a, b, dims):
    return lax.dot_general(a, b, dims, preferred_element_type=F32)


def turn(value, shift):
    shift %= LANES
    return pltpu.roll(value, shift, 1) if shift else value


def up(value, step):
    return -(-value // step) * step


class Plan:
    def __init__(self, tokens, width, block, nb, ns):
        self.tokens, self.width, self.block = tokens, width, block
        self.nb, self.ns = nb, ns
        self.blocks = width // block
        assert self.blocks == 4 and nb % 2 == 0 and nb >= 4 and ns >= 8
        assert LANES < block <= 2 * LANES and block % 8 == 0
        self.tiles = 2 * block // LANES
        self.tail = 2 * block - self.tiles * LANES
        assert 0 < 2 * self.tail <= LANES and LANES % self.tail == 0
        self.fold = LANES // self.tail
        self.fold_rows = up(-(-block // self.fold), 8)
        self.grad_rows = up(block * self.tiles + self.fold_rows, 2 * PACK)
        self.corner = block - LANES
        self.cov_total = up(block + self.corner, PACK)
        units = self.cov_total // PACK
        self.quarter = -(-units // 4)
        self.cuts = [min(units, self.quarter + t * (units - self.quarter) // 3) for t in range(4)]
        self.cuts = [0] + self.cuts
        self.g = self.grad_rows // PACK // 2
        self.c = max(self.cuts[t + 1] - self.cuts[t] for t in range(4))
        self.count = tokens * nb * ns
        self.owned = width // ns

    def lane(self):
        return lax.broadcasted_iota(jnp.int32, (self.block, LANES), 1)

    def pack_pair(self, tiles, h):
        if h == 0:
            sent, rest, start = list(tiles[:-1]), tiles[-1], 0
        else:
            mixed = jnp.where(self.lane() < self.tail, tiles[-1], tiles[0])
            sent, rest, start = [mixed] + list(tiles[1:-1]), tiles[-1], self.tail
        groups = -(-self.block // self.fold_rows)
        short = groups * self.fold_rows - self.block
        if short:
            rest = jnp.concatenate([rest, jnp.zeros((short, LANES), F32)], 0)
        lane = lax.broadcasted_iota(jnp.int32, (self.fold_rows, LANES), 1)
        folded = jnp.zeros((self.fold_rows, LANES), F32)
        for i in range(groups):
            piece = rest[i * self.fold_rows:(i + 1) * self.fold_rows]
            piece = turn(piece, i * self.tail - start)
            folded = jnp.where(lane // self.tail == i, piece, folded)
        stacked = jnp.concatenate(sent + [folded], 0)
        left = self.grad_rows - stacked.shape[0]
        if left:
            stacked = jnp.concatenate([stacked, jnp.zeros((left, LANES), F32)], 0)
        return stacked.reshape(2, self.g, PACK, LANES)

    def unpack_pair(self, packed, h):
        stacked = packed.reshape(self.grad_rows, LANES)
        sent = [stacked[k * self.block:(k + 1) * self.block] for k in range(self.tiles)]
        base = self.tiles * self.block
        folded = stacked[base:base + self.fold_rows]
        groups = -(-self.block // self.fold_rows)
        start = 0 if h == 0 else self.tail
        rest = jnp.concatenate(
            [turn(folded, start - i * self.tail) for i in range(groups)], 0)[:self.block]
        if h == 0:
            return sent + [rest]
        last = jnp.where(self.lane() < self.tail, sent[0], rest)
        return sent + [last]

    def tiles_of(self, rows, h):
        start = h * self.tiles * LANES
        stop = min(start + (self.tiles + 1) * LANES, self.width)
        tiles = [rows[:, at:min(at + LANES, stop)] for at in range(start, stop, LANES)]
        missing = LANES - tiles[-1].shape[1]
        if missing:
            pad = jnp.zeros((self.block, missing), F32)
            tiles[-1] = jnp.concatenate([tiles[-1], pad], 1)
        return tiles

    def pack_cov(self, matrix):
        corner = matrix[LANES:, LANES:]
        corner = jnp.concatenate([corner, jnp.zeros((self.corner, LANES - self.corner), F32)], 1)
        stacked = jnp.concatenate([matrix[:, :LANES], corner], 0)
        left = self.cov_total - stacked.shape[0]
        if left:
            stacked = jnp.concatenate([stacked, jnp.zeros((left, LANES), F32)], 0)
        return stacked.reshape(self.cov_total // PACK, PACK, LANES)


def place(plan):
    batch = lax.axis_index("batch")
    seq = lax.axis_index("seq")
    core = batch % 2
    xy = (batch // 2 % 2) * 2 + seq % 2
    owner_block = seq // (plan.ns // plan.blocks)
    return seq, core, xy, owner_block


def grad_kernel(plan, x_ref, y_ref, keep_ref, send_ref, both_ref, sems):
    _, core, xy, _ = place(plan)
    copies = [
        pltpu.make_async_copy(x_ref, both_ref.at[0], sems.at[0]),
        pltpu.make_async_copy(y_ref, both_ref.at[1], sems.at[1]),
    ]
    for copy in copies:
        copy.start()
    copies[0].wait()
    turned = both_ref[0].T
    copies[1].wait()
    grad = dot(turned, both_ref[1], NN)
    for b in range(plan.blocks):
        rows = grad[b * plan.block:(b + 1) * plan.block]
        for h in range(2):
            packed = plan.pack_pair(plan.tiles_of(rows, h), h)
            j = (b % 2 * 2 + h) ^ xy

            @pl.when(core == b // 2)
            def _():
                keep_ref[j] = packed

            @pl.when(core != b // 2)
            def _():
                send_ref[j] = packed.astype(BF16)


def cov_kernel(plan, mine, both_ref, after_ref, out_ref):
    _, core, xy, owner_block = place(plan)
    block = plan.block
    factor = core if mine else 1 - core
    for b in range(plan.blocks):
        part = both_ref[factor, :, b * block:(b + 1) * block]
        stacked = plan.pack_cov(dot(part, part, TN))
        slot = (b ^ owner_block) * plan.c
        for t in range(4):
            piece = stacked[plan.cuts[t]:plan.cuts[t + 1]]
            out_ref[t ^ xy, pl.ds(slot, piece.shape[0])] = piece.astype(out_ref.dtype)


def split_kernel(keep_ref, recv_ref, after_ref, own_ref, *send_refs):
    own_ref[...] = keep_ref[0] + recv_ref[0].astype(F32)
    for j in range(1, 4):
        send_refs[j - 1][...] = (keep_ref[j] + recv_ref[j].astype(F32)).astype(BF16)


def total(parts, at):
    value = parts[0][at].astype(F32)
    for ref in parts[1:]:
        value = value + ref[at].astype(F32)
    return value


def sum_kernel(*refs):
    refs[-1][...] = total(refs[:-1], ...).astype(refs[-1].dtype)


def first_kernel(plan, parts, outs):
    send_ref, keep_ref = outs
    half = place(plan)[3] % 2
    keep_ref[...] = total(parts[:-1], half)
    send_ref[...] = total(parts[:-1], 1 - half).astype(BF16)


def second_kernel(plan, parts, outs):
    mine_ref, recv_ref, *cov_refs = parts
    send_ref, cov_ref = outs
    g, c = plan.g, plan.c
    send_ref[pl.ds(0, g)] = (mine_ref[...] + recv_ref[...].astype(F32)).astype(BF16)
    cov_ref[...] = total(cov_refs, pl.ds(0, 2 * c))
    send_ref[pl.ds(g, 2 * c)] = total(cov_refs, pl.ds(2 * c, 2 * c)).astype(BF16)


def third_kernel(plan, mine_ref, recv_ref, cov_ref, out_ref, keep_ref):
    g, c = plan.g, plan.c
    out_ref[pl.ds(0, g)] = total((mine_ref, recv_ref), pl.ds(0, g)).astype(BF16)
    other = cov_ref[pl.ds(c, c)] + recv_ref[pl.ds(g + c, c)].astype(F32)
    out_ref[pl.ds(g, c)] = other.astype(BF16)
    keep_ref[...] = cov_ref[pl.ds(0, c)] + recv_ref[pl.ds(g, c)].astype(F32)


def split_two(value):
    high = value.astype(BF16)
    return high, (value - high.astype(F32)).astype(BF16)


def dot_split(a, b, dims):
    a_high, a_low = split_two(a)
    b_high, b_low = split_two(b)
    return dot(a_high, b_high, dims) + (dot(a_high, b_low, dims) + dot(a_low, b_high, dims))


def pick(ref, plan, wanted):
    value = ref[:, :plan.block]
    for n in range(1, plan.blocks):
        value = jnp.where(wanted == n, ref[:, n * plan.block:(n + 1) * plan.block], value)
    return value


def finish_kernel(plan, mine_ref, recv_ref, cov_ref, p_ref, q_ref, out_ref, whole):
    _, core, xy, owner_block = place(plan)
    g, c, block = plan.g, plan.c, plan.block
    cov = cov_ref[...] + recv_ref[pl.ds(g, c)].astype(F32)
    out_ref[pl.ds(2 * g, c)] = cov.astype(BF16)
    whole[owner_block % 2] = mine_ref[pl.ds(0, g)].astype(F32)
    whole[1 - owner_block % 2] = recv_ref[pl.ds(0, g)].astype(F32)
    low = xy % 2 == 0
    pair = whole[...]
    natural = [jnp.concatenate(plan.unpack_pair(pair, h), 1).astype(BF16) for h in range(2)]
    p_high, p_low = split_two(pick(p_ref, plan, core * 2 + xy // 2).T)
    done = []
    for e in range(2):
        at = e * block
        part = jnp.where(low, natural[0][:, at:at + block].astype(F32),
                         natural[1][:, at + plan.tail:at + plan.tail + block].astype(F32))
        part = part.astype(BF16)
        left = dot(p_high, part, NN) + dot(p_low, part, NN)
        done.append(dot_split(left, pick(q_ref, plan, xy % 2 * 2 + e), NT) * (1.0 / plan.count))
    tail = jnp.zeros((block, plan.tail), F32)
    end = jnp.zeros((block, LANES - 2 * plan.tail), F32)
    packed = []
    for h, order in ((0, done + [tail, end]), (1, [tail] + done + [end])):
        row = jnp.concatenate(order, 1)
        tiles = [row[:, k * LANES:(k + 1) * LANES] for k in range(plan.tiles + 1)]
        packed.append(plan.pack_pair(tiles, h))
    packed = jnp.where(low, packed[0], packed[1]).astype(BF16)
    out_ref[pl.ds(0, 2 * g)] = packed.reshape(2 * g, PACK, LANES)


def assemble_kernel(plan, *refs):
    bundles, (in_ref, out_ref, grad_ref, whole, done, sems, out_sems) = refs[:8], refs[8:]
    seq, core, xy, _ = place(plan)
    g, block = plan.g, plan.block
    copies = []
    for i in range(8):
        q = (core ^ (i // 4)) * 4 + (xy ^ (i % 4))
        copies.append(pltpu.make_async_copy(bundles[i], whole.at[q], sems.at[i]))
    for copy in copies:
        copy.start()
    for copy in copies:
        copy.wait()
    writes = []
    for b in range(plan.blocks):
        low, high = (
            plan.unpack_pair(whole[2 * b + h, pl.ds(0, 2 * g)].astype(F32), h) for h in range(2))
        middle = jnp.where(plan.lane() < plan.tail, low[-1], high[0])
        row = low[:-1] + [middle] + high[1:-1] + [high[-1][:, :2 * plan.tail]]
        done[b] = jnp.concatenate(row, 1).astype(BF16)
        write = pltpu.make_async_copy(
            done.at[b], grad_ref.at[pl.ds(b * block, block)], out_sems.at[b])
        write.start()
        writes.append(write)
    first = (seq % (plan.ns // plan.blocks)) * plan.owned
    row = lax.broadcasted_iota(jnp.int32, (plan.owned, block), 0) + first
    column = lax.broadcasted_iota(jnp.int32, (plan.owned, block), 1)
    select = jnp.where(row == column, 1.0, 0.0).astype(BF16)
    r128 = lax.broadcasted_iota(jnp.int32, (LANES, LANES), 0)
    c128 = lax.broadcasted_iota(jnp.int32, (LANES, LANES), 1)
    eye = jnp.where(r128 == c128, 1.0, 0.0).astype(BF16)
    for factor, ref in ((0, in_ref), (1, out_ref)):
        pieces = [
            whole[factor * 4 + t, pl.ds(2 * g, plan.cuts[t + 1] - plan.cuts[t])].astype(F32)
            for t in range(4)
        ]
        stacked = jnp.concatenate(pieces, 0).reshape(plan.cov_total, LANES)
        left = stacked[:block]
        corner = stacked[block:block + plan.corner, :plan.corner]
        top = dot(eye, left[LANES:].astype(BF16), NT)
        right = jnp.concatenate([top, corner], 0)
        both = jnp.concatenate([left, right], 1).astype(BF16)
        ref[...] = dot(both, select, NT) * (1.0 / plan.count)
    for write in writes:
        write.wait()


def call(kernel, shapes, args, scratch=(), hbm_in=0, hbm_out=()):
    vmem = pl.BlockSpec(memory_space=pltpu.VMEM)
    hbm = pl.BlockSpec(memory_space=pltpu.HBM)
    args = [
        pltpu.with_memory_space_constraint(a, pltpu.HBM) if i < hbm_in else a
        for i, a in enumerate(args)
    ]
    return pl.pallas_call(
        kernel,
        out_shape=[jax.ShapeDtypeStruct(s, d) for s, d in shapes],
        in_specs=[hbm if i < hbm_in else vmem for i in range(len(args))],
        out_specs=[hbm if i in hbm_out else vmem for i in range(len(shapes))],
        scratch_shapes=list(scratch),
        compiler_params=pltpu.CompilerParams(vmem_limit_bytes=VMEM_LIMIT),
    )(*args)


def solution(mesh):
    nb, ns = mesh.shape["batch"], mesh.shape["seq"]

    def swap(value, batch_bits, seq_bits):
        pairs = [
            (b * ns + s, (b ^ batch_bits) * ns + (s ^ seq_bits))
            for b in range(nb) for s in range(ns)
        ]
        return lax.ppermute(value, AXES, pairs)

    def shards(layer_inputs, output_grads, input_inverse, output_inverse):
        tokens, width = layer_inputs.shape
        plan = Plan(tokens, width, input_inverse.shape[1], nb, ns)
        g, c = plan.g, plan.c
        step = ns // plan.blocks
        extra = [(bit, 0) for bit in (4, 8, 16, 32, 64) if bit < nb]
        extra += [(0, bit) for bit in (2, 4, 8, 16, 32, 64) if bit < step]

        def bind(kernel):
            def bound(*refs):
                return kernel(plan, *refs)

            return bound

        def group(kernel, outs, *head):
            def bound(*refs):
                return kernel(*head, refs[:-outs], refs[-outs:])

            return bound

        def units(n, dtype, *lead):
            return (*lead, n, PACK, LANES), dtype

        def exchange_parts(keep, send, after, shape):
            own, *sends = call(
                split_kernel, [(shape, F32)] + [(shape, BF16)] * 3,
                (keep, swap(send, 1, 0), after))
            peers = [swap(sends[2], 2, 1), swap(sends[1], 2, 0), swap(sends[0], 0, 1)]
            return [own] + peers

        def widen(parts, shape):
            for batch_bit, seq_bit in extra:
                summed, = call(sum_kernel, [(shape, BF16)], parts)
                parts = [summed, swap(summed, batch_bit, seq_bit)]
            return parts

        tile = (PACK, LANES)
        keep, send, both = call(
            bind(grad_kernel),
            [units(g, F32, 4, 2), units(g, BF16, 4, 2), ((2, tokens, width), BF16)],
            (layer_inputs, output_grads), hbm_in=2,
            scratch=[pltpu.SemaphoreType.DMA((2,))])
        cov_send, = call(
            group(lambda refs, outs: cov_kernel(plan, False, *refs, *outs), 1),
            [units(4 * c, BF16, 4)], (both, send))
        parts = exchange_parts(keep, send, cov_send, (2, g, *tile))
        cov_keep, = call(
            group(lambda refs, outs: cov_kernel(plan, True, *refs, *outs), 1),
            [units(4 * c, F32, 4)], (both, parts[0]))
        cov_parts = exchange_parts(cov_keep, cov_send, parts[0], (4 * c, *tile))
        send, keep = call(
            group(first_kernel, 2, plan), [units(g, BF16), units(g, F32)],
            widen(parts, (2, g, *tile)) + [cov_parts[0]])
        send, cov = call(
            group(second_kernel, 2, plan), [units(g + 2 * c, BF16), units(2 * c, F32)],
            [keep, swap(send, 0, step)] + widen(cov_parts, (4 * c, *tile)))
        send, cov = call(
            bind(third_kernel), [units(g + c, BF16), units(c, F32)],
            (send, swap(send, 0, 2 * step), cov))
        done, = call(
            bind(finish_kernel), [units(2 * g + c, BF16)],
            (send, swap(send, 0, step), cov, input_inverse.T, output_inverse.T),
            scratch=[pltpu.VMEM(units(g, F32, 2)[0], F32)])
        mine = [done, swap(done, 0, 1), swap(done, 2, 0), swap(done, 2, 1)]
        theirs = [swap(value, 1, 0) for value in mine]
        in_factor, out_factor, grad = call(
            bind(assemble_kernel),
            [((plan.block, plan.owned), F32)] * 2 + [((width, width), BF16)],
            mine + theirs, hbm_out=(2,),
            scratch=[
                pltpu.VMEM(units(2 * g + c, BF16, 8)[0], BF16),
                pltpu.VMEM((plan.blocks, plan.block, width), BF16),
                pltpu.SemaphoreType.DMA((8,)), pltpu.SemaphoreType.DMA((plan.blocks,))])
        return in_factor.T, out_factor.T, grad

    return jax.shard_map(
        shards,
        mesh=mesh,
        in_specs=(P(AXES, None), P(AXES, None), P(), P()),
        out_specs=(P("seq", None), P("seq", None), P()),
        check_vma=False,
    )
```

```python
import jax
import jax.numpy as jnp
from jax import lax
from jax.experimental import pallas as pl
from jax.experimental.pallas import tpu as pltpu
from jax.sharding import PartitionSpec as P


AXES = ("batch", "seq")
LANES = 128
PACK = 16
VMEM_LIMIT = 16 << 20
F32 = jnp.float32
BF16 = jnp.bfloat16
NN = (((1,), (0,)), ((), ()))
NT = (((1,), (1,)), ((), ()))
TN = (((0,), (0,)), ((), ()))


def dot(a, b, dims):
    return lax.dot_general(a, b, dims, preferred_element_type=F32)


def turn(value, shift):
    shift %= LANES
    return pltpu.roll(value, shift, 1) if shift else value


def up(value, step):
    return -(-value // step) * step


class Plan:
    def __init__(self, tokens, width, block, nb, ns):
        self.tokens, self.width, self.block = tokens, width, block
        self.nb, self.ns = nb, ns
        self.blocks = width // block
        assert self.blocks == 4 and nb % 2 == 0 and nb >= 4 and ns >= 8
        assert LANES < block <= 2 * LANES and block % 8 == 0
        self.tiles = 2 * block // LANES
        self.tail = 2 * block - self.tiles * LANES
        assert 0 < 2 * self.tail <= LANES and LANES % self.tail == 0
        self.fold = LANES // self.tail
        self.fold_rows = up(-(-block // self.fold), 8)
        self.grad_rows = up(block * self.tiles + self.fold_rows, 2 * PACK)
        self.corner = block - LANES
        self.cov_total = up(block + self.corner, PACK)
        units = self.cov_total // PACK
        self.quarter = -(-units // 4)
        self.cuts = [min(units, self.quarter + t * (units - self.quarter) // 3) for t in range(4)]
        self.cuts = [0] + self.cuts
        self.g = self.grad_rows // PACK // 2
        self.c = max(self.cuts[t + 1] - self.cuts[t] for t in range(4))
        self.count = tokens * nb * ns
        self.owned = width // ns

    def lane(self):
        return lax.broadcasted_iota(jnp.int32, (self.block, LANES), 1)

    def pack_pair(self, tiles, high):
        free = jnp.where(high, self.tail, 0)
        mixed = jnp.where(self.lane() < free, tiles[-1], tiles[0])
        rest = jnp.where(high, turn(tiles[-1], -self.tail), tiles[-1])
        groups = -(-self.block // self.fold_rows)
        short = groups * self.fold_rows - self.block
        if short:
            rest = jnp.concatenate([rest, jnp.zeros((short, LANES), F32)], 0)
        lane = lax.broadcasted_iota(jnp.int32, (self.fold_rows, LANES), 1)
        folded = jnp.zeros((self.fold_rows, LANES), F32)
        for i in range(groups):
            piece = turn(rest[i * self.fold_rows:(i + 1) * self.fold_rows], i * self.tail)
            folded = jnp.where(lane // self.tail == i, piece, folded)
        stacked = jnp.concatenate([mixed] + list(tiles[1:-1]) + [folded], 0)
        left = self.grad_rows - stacked.shape[0]
        if left:
            stacked = jnp.concatenate([stacked, jnp.zeros((left, LANES), F32)], 0)
        return stacked.reshape(2, self.g, PACK, LANES)

    def unpack_pair(self, packed, h):
        stacked = packed.reshape(self.grad_rows, LANES)
        sent = [stacked[k * self.block:(k + 1) * self.block] for k in range(self.tiles)]
        base = self.tiles * self.block
        folded = stacked[base:base + self.fold_rows]
        groups = -(-self.block // self.fold_rows)
        start = 0 if h == 0 else self.tail
        rest = jnp.concatenate(
            [turn(folded, start - i * self.tail) for i in range(groups)], 0)[:self.block]
        if h == 0:
            return sent + [rest]
        last = jnp.where(self.lane() < self.tail, sent[0], rest)
        return sent + [last]

    def pack_cov(self, matrix):
        corner = matrix[LANES:, LANES:]
        corner = jnp.concatenate([corner, jnp.zeros((self.corner, LANES - self.corner), F32)], 1)
        stacked = jnp.concatenate([matrix[:, :LANES], corner], 0)
        left = self.cov_total - stacked.shape[0]
        if left:
            stacked = jnp.concatenate([stacked, jnp.zeros((left, LANES), F32)], 0)
        return stacked.reshape(self.cov_total // PACK, PACK, LANES)


def place(plan):
    batch = lax.axis_index("batch")
    seq = lax.axis_index("seq")
    core = batch % 2
    xy = (batch // 2 % 2) * 2 + seq % 2
    owner_block = seq // (plan.ns // plan.blocks)
    return seq, core, xy, owner_block


def grad_half(plan, other, turned, both_ref, keep_ref, send_ref):
    _, core, xy, _ = place(plan)
    high = (xy + other) % 2 == 1
    span = (plan.tiles + 1) * LANES
    start = plan.tiles * LANES
    late = both_ref[1, :, start:]
    missing = span - late.shape[1]
    if missing:
        late = jnp.concatenate([late, jnp.zeros((plan.tokens, missing), BF16)], 1)
    part = jnp.where(high, late, both_ref[1, :, :span])
    grad = dot(turned, part, NN)
    for b in range(plan.blocks):
        rows = grad[b * plan.block:(b + 1) * plan.block]
        tiles = [rows[:, k * LANES:(k + 1) * LANES] for k in range(plan.tiles + 1)]
        packed = plan.pack_pair(tiles, high)
        j = b % 2 ^ xy // 2

        @pl.when(core == b // 2)
        def _():
            keep_ref[j] = packed

        @pl.when(core != b // 2)
        def _():
            send_ref[j] = packed.astype(BF16)


def far_kernel(plan, x_ref, y_ref, keep_ref, send_ref, both_ref, turned_ref, sems):
    copies = [
        pltpu.make_async_copy(x_ref, both_ref.at[0], sems.at[0]),
        pltpu.make_async_copy(y_ref, both_ref.at[1], sems.at[1]),
    ]
    for copy in copies:
        copy.start()
    copies[0].wait()
    turned = both_ref[0].T
    turned_ref[...] = turned
    copies[1].wait()
    grad_half(plan, 1, turned, both_ref, keep_ref, send_ref)


def near_kernel(plan, both_ref, turned_ref, keep_ref, send_ref):
    grad_half(plan, 0, turned_ref[...], both_ref, keep_ref, send_ref)


def cov_kernel(plan, mine, both_ref, after_ref, out_ref):
    _, core, xy, owner_block = place(plan)
    block = plan.block
    factor = core if mine else 1 - core
    for b in range(plan.blocks):
        part = both_ref[factor, :, b * block:(b + 1) * block]
        stacked = plan.pack_cov(dot(part, part, TN))
        slot = (b ^ owner_block) * plan.c
        for t in range(4):
            piece = stacked[plan.cuts[t]:plan.cuts[t + 1]]
            out_ref[t ^ xy, pl.ds(slot, piece.shape[0])] = piece.astype(out_ref.dtype)


def far_split_kernel(keep_ref, recv_ref, after_ref, y_ref, d_ref):
    for j, ref in enumerate((y_ref, d_ref)):
        ref[...] = (keep_ref[j] + recv_ref[j].astype(F32)).astype(BF16)


def near_split_kernel(keep_ref, recv_ref, after_ref, own_ref, x_ref):
    own_ref[...] = keep_ref[0] + recv_ref[0].astype(F32)
    x_ref[...] = (keep_ref[1] + recv_ref[1].astype(F32)).astype(BF16)


def split_kernel(keep_ref, recv_ref, after_ref, own_ref, *send_refs):
    own_ref[...] = keep_ref[0] + recv_ref[0].astype(F32)
    for j in range(1, 4):
        send_refs[j - 1][...] = (keep_ref[j] + recv_ref[j].astype(F32)).astype(BF16)


def total(parts, at):
    value = parts[0][at].astype(F32)
    for ref in parts[1:]:
        value = value + ref[at].astype(F32)
    return value


def sum_kernel(*refs):
    refs[-1][...] = total(refs[:-1], ...).astype(refs[-1].dtype)


def first_kernel(plan, parts, outs):
    send_ref, keep_ref = outs
    half = place(plan)[3] % 2
    keep_ref[...] = total(parts[:-1], half)
    send_ref[...] = total(parts[:-1], 1 - half).astype(BF16)


def second_kernel(plan, parts, outs):
    mine_ref, recv_ref, *cov_refs = parts
    send_ref, cov_ref = outs
    g, c = plan.g, plan.c
    send_ref[pl.ds(0, g)] = (mine_ref[...] + recv_ref[...].astype(F32)).astype(BF16)
    cov_ref[...] = total(cov_refs, pl.ds(0, 2 * c))
    send_ref[pl.ds(g, 2 * c)] = total(cov_refs, pl.ds(2 * c, 2 * c)).astype(BF16)


def third_kernel(plan, mine_ref, recv_ref, cov_ref, out_ref, keep_ref):
    g, c = plan.g, plan.c
    out_ref[pl.ds(0, g)] = total((mine_ref, recv_ref), pl.ds(0, g)).astype(BF16)
    other = cov_ref[pl.ds(c, c)] + recv_ref[pl.ds(g + c, c)].astype(F32)
    out_ref[pl.ds(g, c)] = other.astype(BF16)
    keep_ref[...] = cov_ref[pl.ds(0, c)] + recv_ref[pl.ds(g, c)].astype(F32)


def split_two(value):
    high = value.astype(BF16)
    return high, (value - high.astype(F32)).astype(BF16)


def pick(ref, plan, wanted):
    value = ref[:, :plan.block]
    for n in range(1, plan.blocks):
        value = jnp.where(wanted == n, ref[:, n * plan.block:(n + 1) * plan.block], value)
    return value


def inverses_kernel(plan, p_ref, q_ref, after_ref, p_out, q_out):
    _, core, xy, _ = place(plan)
    high, low = split_two(pick(p_ref, plan, core * 2 + xy // 2).T)
    p_out[0], p_out[1] = high, low
    for e in range(2):
        high, low = split_two(pick(q_ref, plan, xy % 2 * 2 + e))
        q_out[e, 0], q_out[e, 1] = high, low


def finish_kernel(plan, mine_ref, recv_ref, cov_ref, p_ref, q_ref, out_ref, whole):
    _, _, xy, owner_block = place(plan)
    g, c, block = plan.g, plan.c, plan.block
    cov = cov_ref[...] + recv_ref[pl.ds(g, c)].astype(F32)
    out_ref[pl.ds(2 * g, c)] = cov.astype(BF16)
    whole[owner_block % 2] = mine_ref[pl.ds(0, g)].astype(F32)
    whole[1 - owner_block % 2] = recv_ref[pl.ds(0, g)].astype(F32)
    high = xy % 2 == 1
    pair = whole[...]
    natural = [jnp.concatenate(plan.unpack_pair(pair, h), 1) for h in range(2)]
    part = jnp.where(high, natural[1][:, plan.tail:plan.tail + 2 * block],
                     natural[0][:, :2 * block]).astype(BF16)
    left = dot(p_ref[0], part, NN) + dot(p_ref[1], part, NN)
    done = []
    for e in range(2):
        l_high, l_low = split_two(left[:, e * block:(e + 1) * block])
        value = dot(l_high, q_ref[e, 0], NT) + (
            dot(l_high, q_ref[e, 1], NT) + dot(l_low, q_ref[e, 0], NT))
        done.append(value * (1.0 / plan.count))
    tail = jnp.zeros((block, plan.tail), F32)
    end = jnp.zeros((block, LANES - 2 * plan.tail), F32)
    row = jnp.where(high, jnp.concatenate([tail] + done + [end], 1),
                    jnp.concatenate(done + [tail, end], 1))
    tiles = [row[:, k * LANES:(k + 1) * LANES] for k in range(plan.tiles + 1)]
    packed = plan.pack_pair(tiles, high).astype(BF16)
    out_ref[pl.ds(0, 2 * g)] = packed.reshape(2 * g, PACK, LANES)


def assemble(plan, away, bundles, grad_ref, covs, done, sems):
    seq, core, xy, _ = place(plan)
    g, c, block = plan.g, plan.c, plan.block
    even = xy % 2 == 0
    writes = []
    for k in range(2):
        first, second = (bundles[2 * k + e][pl.ds(0, 2 * g)] for e in range(2))
        low = plan.unpack_pair(jnp.where(even, first, second).astype(F32), 0)
        high = plan.unpack_pair(jnp.where(even, second, first).astype(F32), 1)
        middle = jnp.where(plan.lane() < plan.tail, low[-1], high[0])
        row = low[:-1] + [middle] + high[1:-1] + [high[-1][:, :2 * plan.tail]]
        done[k] = jnp.concatenate(row, 1).astype(BF16)
        b = (core ^ away) * 2 + (xy // 2 ^ k)
        write = pltpu.make_async_copy(
            done.at[k], grad_ref.at[pl.ds(pl.multiple_of(b * block, 8), block)], sems.at[k])
        write.start()
        writes.append(write)
    for j in range(4):
        covs[j ^ xy] = bundles[j][pl.ds(2 * g, c)]
    start = (seq % (plan.ns // plan.blocks)) * plan.owned
    row = lax.broadcasted_iota(jnp.int32, (plan.owned, block), 0) + start
    column = lax.broadcasted_iota(jnp.int32, (plan.owned, block), 1)
    select = jnp.where(row == column, 1.0, 0.0).astype(BF16)
    r128 = lax.broadcasted_iota(jnp.int32, (LANES, LANES), 0)
    c128 = lax.broadcasted_iota(jnp.int32, (LANES, LANES), 1)
    eye = jnp.where(r128 == c128, 1.0, 0.0).astype(BF16)
    pieces = [covs[t, pl.ds(0, plan.cuts[t + 1] - plan.cuts[t])].astype(F32) for t in range(4)]
    stacked = jnp.concatenate(pieces, 0).reshape(plan.cov_total, LANES)
    left = stacked[:block]
    corner = stacked[block:block + plan.corner, :plan.corner]
    top = dot(eye, left[LANES:].astype(BF16), NT)
    right = jnp.concatenate([top, corner], 0)
    whole = jnp.concatenate([left, right], 1).astype(BF16)
    factor = dot(whole, select, NT) * (1.0 / plan.count)
    return factor, writes


def home_kernel(plan, *refs):
    bundles, (grad_ref, factor_ref, covs, done, sems) = refs[:4], refs[4:]
    factor_ref[...], writes = assemble(plan, 0, bundles, grad_ref, covs, done, sems)
    for write in writes:
        write.wait()


def away_kernel(plan, *refs):
    _, mine_ref, *bundles = refs[:6]
    grad_ref, in_ref, out_ref, covs, done, sems = refs[6:]
    core = place(plan)[1]
    mine = mine_ref[...]
    theirs, writes = assemble(plan, 1, bundles, grad_ref, covs, done, sems)
    in_ref[...] = jnp.where(core == 0, mine, theirs)
    out_ref[...] = jnp.where(core == 0, theirs, mine)
    for write in writes:
        write.wait()


def call(kernel, shapes, args, scratch=(), hbm_in=0, hbm_out=0, aliases=None):
    vmem = pl.BlockSpec(memory_space=pltpu.VMEM)
    hbm = pl.BlockSpec(memory_space=pltpu.HBM)
    args = [
        pltpu.with_memory_space_constraint(a, pltpu.HBM) if i < hbm_in else a
        for i, a in enumerate(args)
    ]
    return pl.pallas_call(
        kernel,
        out_shape=[jax.ShapeDtypeStruct(s, d) for s, d in shapes],
        in_specs=[hbm if i < hbm_in else vmem for i in range(len(args))],
        out_specs=[hbm if i < hbm_out else vmem for i in range(len(shapes))],
        scratch_shapes=list(scratch),
        compiler_params=pltpu.CompilerParams(vmem_limit_bytes=VMEM_LIMIT),
        input_output_aliases=aliases or {},
    )(*args)


def solution(mesh):
    nb, ns = mesh.shape["batch"], mesh.shape["seq"]

    def swap(value, batch_bits, seq_bits):
        pairs = [
            (b * ns + s, (b ^ batch_bits) * ns + (s ^ seq_bits))
            for b in range(nb) for s in range(ns)
        ]
        return lax.ppermute(value, AXES, pairs)

    def shards(layer_inputs, output_grads, input_inverse, output_inverse):
        tokens, width = layer_inputs.shape
        plan = Plan(tokens, width, input_inverse.shape[1], nb, ns)
        g, c = plan.g, plan.c
        step = ns // plan.blocks
        extra = [(bit, 0) for bit in (4, 8, 16, 32, 64) if bit < nb]
        extra += [(0, bit) for bit in (2, 4, 8, 16, 32, 64) if bit < step]

        def bind(kernel):
            def bound(*refs):
                return kernel(plan, *refs)

            return bound

        def group(kernel, outs, *head):
            def bound(*refs):
                return kernel(*head, refs[:-outs], refs[-outs:])

            return bound

        def units(n, dtype, *lead):
            return (*lead, n, PACK, LANES), dtype

        def widen(parts, shape):
            for batch_bit, seq_bit in extra:
                summed, = call(sum_kernel, [(shape, BF16)], parts)
                parts = [summed, swap(summed, batch_bit, seq_bit)]
            return parts

        tile = (PACK, LANES)
        far_keep, far_send, both, turned = call(
            bind(far_kernel),
            [units(g, F32, 2, 2), units(g, BF16, 2, 2), ((2, tokens, width), BF16),
             ((width, tokens), BF16)],
            (layer_inputs, output_grads), hbm_in=2,
            scratch=[pltpu.SemaphoreType.DMA((2,))])
        far_recv = swap(far_send, 1, 0)
        near_keep, near_send = call(
            bind(near_kernel), [units(g, F32, 2, 2), units(g, BF16, 2, 2)],
            (both, turned))
        near_recv = swap(near_send, 1, 0)
        y_send, d_send = call(
            far_split_kernel, [units(g, BF16, 2)] * 2,
            (far_keep, far_recv, near_send))
        y_recv, d_recv = swap(y_send, 0, 1), swap(d_send, 2, 1)
        own, x_send = call(
            near_split_kernel, [units(g, F32, 2), units(g, BF16, 2)],
            (near_keep, near_recv, y_send))
        x_recv = swap(x_send, 2, 0)
        parts = [own, y_recv, d_recv, x_recv]
        cov_send, = call(
            group(lambda refs, outs: cov_kernel(plan, False, *refs, *outs), 1),
            [units(4 * c, BF16, 4)], (both, own))
        cov_recv = swap(cov_send, 1, 0)
        cov_keep, = call(
            group(lambda refs, outs: cov_kernel(plan, True, *refs, *outs), 1),
            [units(4 * c, F32, 4)], (both, cov_send))
        cov_own, *cov_sends = call(
            split_kernel, [units(4 * c, F32)] + [units(4 * c, BF16)] * 3,
            (cov_keep, cov_recv, own))
        cov_parts = [cov_own, swap(cov_sends[0], 0, 1), swap(cov_sends[1], 2, 0),
                     swap(cov_sends[2], 2, 1)]
        send, keep = call(
            group(first_kernel, 2, plan), [units(g, BF16), units(g, F32)],
            widen(parts, (2, g, *tile)) + [cov_parts[0]])
        send, cov = call(
            group(second_kernel, 2, plan), [units(g + 2 * c, BF16), units(2 * c, F32)],
            [keep, swap(send, 0, step)] + widen(cov_parts, (4 * c, *tile)))
        send, cov = call(
            bind(third_kernel), [units(g + c, BF16), units(c, F32)],
            (send, swap(send, 0, 2 * step), cov))
        p_parts, q_parts = call(
            bind(inverses_kernel),
            [((2, plan.block, plan.block), BF16), ((2, 2, plan.block, plan.block), BF16)],
            (input_inverse.T, output_inverse.T, keep))
        done, = call(
            bind(finish_kernel), [units(2 * g + c, BF16)],
            (send, swap(send, 0, step), cov, p_parts, q_parts),
            scratch=[pltpu.VMEM(units(g, F32, 2)[0], F32)])
        mine = [done, swap(done, 0, 1), swap(done, 2, 0), swap(done, 2, 1)]
        theirs = [swap(value, 1, 0) for value in mine]
        staging = [
            pltpu.VMEM(units(c, BF16, 4)[0], BF16), pltpu.VMEM((2, plan.block, width), BF16),
            pltpu.SemaphoreType.DMA((2,))]
        result, factor = ((width, width), BF16), ((plan.block, plan.owned), F32)
        grad, home = call(
            bind(home_kernel), [result, factor], mine, hbm_out=1, scratch=staging)
        grad, in_factor, out_factor = call(
            bind(away_kernel), [result, factor, factor], [grad, home] + theirs,
            hbm_in=1, hbm_out=1, aliases={0: 0}, scratch=staging)
        return in_factor.T, out_factor.T, grad

    return jax.shard_map(
        shards,
        mesh=mesh,
        in_specs=(P(AXES, None), P(AXES, None), P(), P()),
        out_specs=(P("seq", None), P("seq", None), P()),
        check_vma=False,
    )
```

```python
import jax
import jax.numpy as jnp
from jax import lax
from jax.experimental import pallas as pl
from jax.experimental.pallas import tpu as pltpu
from jax.sharding import PartitionSpec as P


AXES = ("batch", "seq")
LANES = 128
PACK = 16
VMEM_LIMIT = 16 << 20
F32 = jnp.float32
BF16 = jnp.bfloat16
NN = (((1,), (0,)), ((), ()))
NT = (((1,), (1,)), ((), ()))
TN = (((0,), (0,)), ((), ()))


def dot(a, b, dims):
    return lax.dot_general(a, b, dims, preferred_element_type=F32)


def turn(value, shift):
    shift %= LANES
    return pltpu.roll(value, shift, 1) if shift else value


def up(value, step):
    return -(-value // step) * step


class Plan:
    def __init__(self, tokens, width, block, nb, ns):
        self.tokens, self.width, self.block = tokens, width, block
        self.nb, self.ns = nb, ns
        self.blocks = width // block
        assert self.blocks == 4 and nb % 2 == 0 and nb >= 4 and ns >= 8
        assert LANES < block <= 2 * LANES and block % 8 == 0
        self.tiles = 2 * block // LANES
        self.tail = 2 * block - self.tiles * LANES
        assert 0 < 2 * self.tail <= LANES and LANES % self.tail == 0
        self.fold = LANES // self.tail
        self.fold_rows = up(-(-block // self.fold), 8)
        self.grad_rows = up(block * self.tiles + self.fold_rows, 2 * PACK)
        self.corner = up(block // 2, 8)
        assert self.corner < LANES and block - self.corner < self.corner + 1
        self.cov_total = up(block, PACK)
        units = self.cov_total // PACK
        self.quarter = -(-units // 4)
        self.cuts = [min(units, self.quarter + t * (units - self.quarter) // 3) for t in range(4)]
        self.cuts = [0] + self.cuts
        self.g = self.grad_rows // PACK // 2
        self.c = max(self.cuts[t + 1] - self.cuts[t] for t in range(4))
        self.count = tokens * nb * ns
        self.owned = width // ns

    def lane(self):
        return lax.broadcasted_iota(jnp.int32, (self.block, LANES), 1)

    def pack_pair(self, tiles, high):
        free = jnp.where(high, self.tail, 0)
        mixed = jnp.where(self.lane() < free, tiles[-1], tiles[0])
        rest = jnp.where(high, turn(tiles[-1], -self.tail), tiles[-1])
        groups = -(-self.block // self.fold_rows)
        short = groups * self.fold_rows - self.block
        if short:
            rest = jnp.concatenate([rest, jnp.zeros((short, LANES), F32)], 0)
        lane = lax.broadcasted_iota(jnp.int32, (self.fold_rows, LANES), 1)
        folded = jnp.zeros((self.fold_rows, LANES), F32)
        for i in range(groups):
            piece = turn(rest[i * self.fold_rows:(i + 1) * self.fold_rows], i * self.tail)
            folded = jnp.where(lane // self.tail == i, piece, folded)
        stacked = jnp.concatenate([mixed] + list(tiles[1:-1]) + [folded], 0)
        left = self.grad_rows - stacked.shape[0]
        if left:
            stacked = jnp.concatenate([stacked, jnp.zeros((left, LANES), F32)], 0)
        return stacked.reshape(2, self.g, PACK, LANES)

    def unpack_pair(self, packed, h):
        stacked = packed.reshape(self.grad_rows, LANES)
        sent = [stacked[k * self.block:(k + 1) * self.block] for k in range(self.tiles)]
        base = self.tiles * self.block
        folded = stacked[base:base + self.fold_rows]
        groups = -(-self.block // self.fold_rows)
        start = 0 if h == 0 else self.tail
        rest = jnp.concatenate(
            [turn(folded, start - i * self.tail) for i in range(groups)], 0)[:self.block]
        if h == 0:
            return sent + [rest]
        last = jnp.where(self.lane() < self.tail, sent[0], rest)
        return sent + [last]

    def below(self):
        shape = (self.corner, LANES)
        row = lax.broadcasted_iota(jnp.int32, shape, 0)
        return lax.broadcasted_iota(jnp.int32, shape, 1) <= row

    def pack_cov(self, matrix):
        n, m = self.corner, self.block - self.corner
        late = jnp.concatenate([matrix[n:, LANES:], jnp.zeros((m, 2 * LANES - self.block), F32)], 1)
        lane = lax.broadcasted_iota(jnp.int32, (m, LANES), 1)
        second = jnp.where(lane < LANES - n + 1, turn(matrix[n:, :LANES], 1 - n), turn(late, 1 - n))
        if n > m:
            second = jnp.concatenate([second, jnp.zeros((n - m, LANES), F32)], 0)
        merged = jnp.where(self.below(), matrix[:n, :LANES], second)
        stacked = jnp.concatenate([merged, matrix[n:, :LANES]], 0)
        left = self.cov_total - stacked.shape[0]
        if left:
            stacked = jnp.concatenate([stacked, jnp.zeros((left, LANES), F32)], 0)
        return stacked.reshape(self.cov_total // PACK, PACK, LANES)

    def unpack_cov(self, stacked):
        n, m = self.corner, self.block - self.corner
        r128 = lax.broadcasted_iota(jnp.int32, (LANES, LANES), 0)
        c128 = lax.broadcasted_iota(jnp.int32, (LANES, LANES), 1)
        eye = jnp.where(r128 == c128, 1.0, 0.0).astype(BF16)
        merged, lower = stacked[:n], stacked[n:self.block]
        turned = dot(eye, stacked[:self.block].astype(BF16), NT)
        first = jnp.where(self.below()[:, :n], merged[:, :n], turned[:n, :n])
        row = lax.broadcasted_iota(jnp.int32, (m, m), 0)
        upper = lax.broadcasted_iota(jnp.int32, (m, m), 1) >= row
        second = jnp.where(upper, merged[:m, 1:m + 1], turned[1:m + 1, :m])
        top = jnp.concatenate([first, turned[:n, n:self.block]], 1)
        bottom = jnp.concatenate([lower[:, :n], second], 1)
        return jnp.concatenate([top, bottom], 0)


def place(plan):
    batch = lax.axis_index("batch")
    seq = lax.axis_index("seq")
    core = batch % 2
    xy = (batch // 2 % 2) * 2 + seq % 2
    owner_block = seq // (plan.ns // plan.blocks)
    return seq, core, xy, owner_block


def grad_half(plan, other, turned, both_ref, keep_ref, send_ref):
    _, core, xy, _ = place(plan)
    high = (xy + other) % 2 == 1
    span = (plan.tiles + 1) * LANES
    start = plan.tiles * LANES
    late = both_ref[1, :, start:]
    missing = span - late.shape[1]
    if missing:
        late = jnp.concatenate([late, jnp.zeros((plan.tokens, missing), BF16)], 1)
    part = jnp.where(high, late, both_ref[1, :, :span])
    grad = dot(turned, part, NN)
    for b in range(plan.blocks):
        rows = grad[b * plan.block:(b + 1) * plan.block]
        tiles = [rows[:, k * LANES:(k + 1) * LANES] for k in range(plan.tiles + 1)]
        packed = plan.pack_pair(tiles, high)
        j = b % 2 ^ xy // 2

        @pl.when(core == b // 2)
        def _():
            keep_ref[j] = packed

        @pl.when(core != b // 2)
        def _():
            send_ref[j] = packed.astype(BF16)


def load_kernel(plan, x_ref, y_ref, keep_ref, send_ref, both_ref, turned_ref, sems):
    copies = [
        pltpu.make_async_copy(x_ref, both_ref.at[0], sems.at[0]),
        pltpu.make_async_copy(y_ref, both_ref.at[1], sems.at[1]),
    ]
    for copy in copies:
        copy.start()
    copies[0].wait()
    turned = both_ref[0].T
    turned_ref[...] = turned
    copies[1].wait()
    grad_half(plan, 1, turned, both_ref, keep_ref, send_ref)


def near_kernel(plan, both_ref, turned_ref, keep_ref, send_ref):
    grad_half(plan, 0, turned_ref[...], both_ref, keep_ref, send_ref)


def cov_kernel(plan, mine, both_ref, after_ref, out_ref):
    _, core, xy, owner_block = place(plan)
    block = plan.block
    factor = core if mine else 1 - core
    for b in range(plan.blocks):
        part = both_ref[factor, :, b * block:(b + 1) * block]
        stacked = plan.pack_cov(dot(part, part, TN))
        slot = (b ^ owner_block) * plan.c
        for t in range(4):
            piece = stacked[plan.cuts[t]:plan.cuts[t + 1]]
            out_ref[t ^ xy, pl.ds(slot, piece.shape[0])] = piece.astype(out_ref.dtype)


def far_split_kernel(keep_ref, recv_ref, after_ref, y_ref, d_ref):
    for j, ref in enumerate((y_ref, d_ref)):
        ref[...] = (keep_ref[j] + recv_ref[j].astype(F32)).astype(BF16)


def near_split_kernel(keep_ref, recv_ref, after_ref, own_ref, x_ref):
    own_ref[...] = keep_ref[0] + recv_ref[0].astype(F32)
    x_ref[...] = (keep_ref[1] + recv_ref[1].astype(F32)).astype(BF16)


def split_kernel(keep_ref, recv_ref, after_ref, own_ref, *send_refs):
    own_ref[...] = keep_ref[0] + recv_ref[0].astype(F32)
    for j in range(1, 4):
        send_refs[j - 1][...] = (keep_ref[j] + recv_ref[j].astype(F32)).astype(BF16)


def total(parts, at):
    value = parts[0][at].astype(F32)
    for ref in parts[1:]:
        value = value + ref[at].astype(F32)
    return value


def sum_kernel(*refs):
    refs[-1][...] = total(refs[:-1], ...).astype(refs[-1].dtype)


def first_kernel(plan, parts, outs):
    send_ref, keep_ref = outs
    half = place(plan)[3] % 2
    keep_ref[...] = total(parts[:-1], half)
    send_ref[...] = total(parts[:-1], 1 - half).astype(BF16)


def cov_first_kernel(plan, parts, outs):
    send_ref, keep_ref = outs
    keep_ref[...] = total(parts, pl.ds(0, 2 * plan.c))
    send_ref[...] = total(parts, pl.ds(2 * plan.c, 2 * plan.c)).astype(BF16)


def cov_second_kernel(plan, mine_ref, recv_ref, send_ref, keep_ref):
    c = plan.c
    send_ref[...] = (mine_ref[pl.ds(c, c)] + recv_ref[pl.ds(c, c)].astype(F32)).astype(BF16)
    keep_ref[...] = mine_ref[pl.ds(0, c)] + recv_ref[pl.ds(0, c)].astype(F32)


def split_two(value):
    high = value.astype(BF16)
    return high, (value - high.astype(F32)).astype(BF16)


def pick(ref, plan, wanted):
    value = ref[:, :plan.block]
    for n in range(1, plan.blocks):
        value = jnp.where(wanted == n, ref[:, n * plan.block:(n + 1) * plan.block], value)
    return value


def inverses_kernel(plan, p_ref, q_ref, after_ref, p_out, q_out):
    _, core, xy, _ = place(plan)
    high, low = split_two(pick(p_ref, plan, core * 2 + xy // 2).T)
    p_out[0], p_out[1] = high, low
    for e in range(2):
        high, low = split_two(pick(q_ref, plan, xy % 2 * 2 + e))
        q_out[e, 0], q_out[e, 1] = high, low


def finish_kernel(plan, mine_ref, recv_ref, p_ref, q_ref, out_ref, whole):
    _, _, xy, owner_block = place(plan)
    g, block = plan.g, plan.block
    whole[owner_block % 2] = mine_ref[...].astype(F32)
    whole[1 - owner_block % 2] = recv_ref[...].astype(F32)
    high = xy % 2 == 1
    pair = whole[...]
    natural = [jnp.concatenate(plan.unpack_pair(pair, h), 1) for h in range(2)]
    part = jnp.where(high, natural[1][:, plan.tail:plan.tail + 2 * block],
                     natural[0][:, :2 * block]).astype(BF16)
    left = dot(p_ref[0], part, NN) + dot(p_ref[1], part, NN)
    done = []
    for e in range(2):
        l_high, l_low = split_two(left[:, e * block:(e + 1) * block])
        value = dot(l_high, q_ref[e, 0], NT) + (
            dot(l_high, q_ref[e, 1], NT) + dot(l_low, q_ref[e, 0], NT))
        done.append(value * (1.0 / plan.count))
    tail = jnp.zeros((block, plan.tail), F32)
    end = jnp.zeros((block, LANES - 2 * plan.tail), F32)
    row = jnp.where(high, jnp.concatenate([tail] + done + [end], 1),
                    jnp.concatenate(done + [tail, end], 1))
    tiles = [row[:, k * LANES:(k + 1) * LANES] for k in range(plan.tiles + 1)]
    packed = plan.pack_pair(tiles, high).astype(BF16)
    out_ref[...] = packed.reshape(2 * g, PACK, LANES)


def put_rows(plan, b, bundles, grad_ref, done, sem):
    even = place(plan)[2] % 2 == 0
    first, second = (bundle[...] for bundle in bundles)
    low = plan.unpack_pair(jnp.where(even, first, second).astype(F32), 0)
    high = plan.unpack_pair(jnp.where(even, second, first).astype(F32), 1)
    middle = jnp.where(plan.lane() < plan.tail, low[-1], high[0])
    row = low[:-1] + [middle] + high[1:-1] + [high[-1][:, :2 * plan.tail]]
    done[...] = jnp.concatenate(row, 1).astype(BF16)
    start = pl.multiple_of(b * plan.block, 8)
    write = pltpu.make_async_copy(done, grad_ref.at[pl.ds(start, plan.block)], sem)
    write.start()
    return write


def join_kernel(plan, *refs):
    xy = place(plan)[2]
    for j, ref in enumerate(refs[:4]):
        refs[4][j ^ xy] = ref[...]


def factor_of(plan, covs_ref):
    seq = place(plan)[0]
    start = (seq % (plan.ns // plan.blocks)) * plan.owned
    row = lax.broadcasted_iota(jnp.int32, (plan.owned, plan.block), 0) + start
    column = lax.broadcasted_iota(jnp.int32, (plan.owned, plan.block), 1)
    select = jnp.where(row == column, 1.0, 0.0).astype(BF16)
    pieces = [
        covs_ref[t, pl.ds(0, plan.cuts[t + 1] - plan.cuts[t])].astype(F32) for t in range(4)]
    whole = plan.unpack_cov(jnp.concatenate(pieces, 0).reshape(plan.cov_total, LANES))
    return dot(whole.astype(BF16), select, NT) * (1.0 / plan.count)


def factors_kernel(plan, home_ref, away_ref, in_ref, out_ref):
    core = place(plan)[1]
    home, away = factor_of(plan, home_ref), factor_of(plan, away_ref)
    in_ref[...] = jnp.where(core == 0, home, away)
    out_ref[...] = jnp.where(core == 0, away, home)


def early_kernel(plan, *refs):
    bundles, (grad_ref, home, home_sem, away, away_sem) = refs[:4], refs[4:]
    _, core, xy, _ = place(plan)
    writes = [
        put_rows(plan, core * 2 + xy // 2, bundles[:2], grad_ref, home, home_sem),
        put_rows(plan, 2 - core * 2 + xy // 2, bundles[2:], grad_ref, away, away_sem),
    ]
    for write in writes:
        write.wait()


def late_kernel(plan, away, _, x_ref, d_ref, grad_ref, done, sem):
    _, core, xy, _ = place(plan)
    b = (core ^ away) * 2 + 1 - xy // 2
    put_rows(plan, b, (x_ref, d_ref), grad_ref, done, sem).wait()


def call(kernel, shapes, args, scratch=(), hbm_in=0, hbm_out=0, aliases=None):
    vmem = pl.BlockSpec(memory_space=pltpu.VMEM)
    hbm = pl.BlockSpec(memory_space=pltpu.HBM)
    args = [
        pltpu.with_memory_space_constraint(a, pltpu.HBM) if i < hbm_in else a
        for i, a in enumerate(args)
    ]
    return pl.pallas_call(
        kernel,
        out_shape=[jax.ShapeDtypeStruct(s, d) for s, d in shapes],
        in_specs=[hbm if i < hbm_in else vmem for i in range(len(args))],
        out_specs=[hbm if i < hbm_out else vmem for i in range(len(shapes))],
        scratch_shapes=list(scratch),
        compiler_params=pltpu.CompilerParams(vmem_limit_bytes=VMEM_LIMIT),
        input_output_aliases=aliases or {},
    )(*args)


def solution(mesh):
    nb, ns = mesh.shape["batch"], mesh.shape["seq"]

    def swap(value, batch_bits, seq_bits):
        pairs = [
            (b * ns + s, (b ^ batch_bits) * ns + (s ^ seq_bits))
            for b in range(nb) for s in range(ns)
        ]
        return lax.ppermute(value, AXES, pairs)

    def shards(layer_inputs, output_grads, input_inverse, output_inverse):
        tokens, width = layer_inputs.shape
        plan = Plan(tokens, width, input_inverse.shape[1], nb, ns)
        g, c = plan.g, plan.c
        step = ns // plan.blocks
        extra = [(bit, 0) for bit in (4, 8, 16, 32, 64) if bit < nb]
        extra += [(0, bit) for bit in (2, 4, 8, 16, 32, 64) if bit < step]

        def bind(kernel):
            def bound(*refs):
                return kernel(plan, *refs)

            return bound

        def group(kernel, outs, *head):
            def bound(*refs):
                return kernel(*head, refs[:-outs], refs[-outs:])

            return bound

        def units(n, dtype, *lead):
            return (*lead, n, PACK, LANES), dtype

        def widen(parts, shape):
            for batch_bit, seq_bit in extra:
                summed, = call(sum_kernel, [(shape, BF16)], parts)
                parts = [summed, swap(summed, batch_bit, seq_bit)]
            return parts

        tile = (PACK, LANES)
        far_keep, far_send, both, turned = call(
            bind(load_kernel),
            [units(g, F32, 2, 2), units(g, BF16, 2, 2), ((2, tokens, width), BF16),
             ((width, tokens), BF16)],
            (layer_inputs, output_grads), hbm_in=2,
            scratch=[pltpu.SemaphoreType.DMA((2,))])
        far_recv = swap(far_send, 1, 0)
        near_keep, near_send = call(
            bind(near_kernel), [units(g, F32, 2, 2), units(g, BF16, 2, 2)],
            (both, turned))
        near_recv = swap(near_send, 1, 0)
        y_send, d_send = call(
            far_split_kernel, [units(g, BF16, 2)] * 2,
            (far_keep, far_recv, near_send))
        d_recv = swap(d_send, 2, 1)
        y_recv = swap(y_send, 0, 1)
        own, x_send = call(
            near_split_kernel, [units(g, F32, 2), units(g, BF16, 2)],
            (near_keep, near_recv, y_send))
        x_recv = swap(x_send, 2, 0)
        parts = [own, x_recv, y_recv, d_recv]
        cov_send, = call(
            group(lambda refs, outs: cov_kernel(plan, False, *refs, *outs), 1),
            [units(4 * c, BF16, 4)], (both, own))
        cov_recv = swap(cov_send, 1, 0)
        cov_keep, = call(
            group(lambda refs, outs: cov_kernel(plan, True, *refs, *outs), 1),
            [units(4 * c, F32, 4)], (both, cov_send))
        cov_own, *cov_sends = call(
            split_kernel, [units(4 * c, F32)] + [units(4 * c, BF16)] * 3,
            (cov_keep, cov_recv, own))
        cov_parts = [
            cov_own, swap(cov_sends[0], 0, 1),
            swap(cov_sends[1], 2, 0),
            swap(cov_sends[2], 2, 1)]
        send, keep = call(
            group(first_kernel, 2, plan), [units(g, BF16), units(g, F32)],
            widen(parts, (2, g, *tile)) + [cov_own])
        recv = swap(send, 0, step)
        send, = call(sum_kernel, [units(g, BF16)], (keep, recv))
        recv = swap(send, 0, 2 * step)
        cov_send, cov = call(
            group(cov_first_kernel, 2, plan), [units(2 * c, BF16), units(2 * c, F32)],
            widen(cov_parts, (4 * c, *tile)))
        cov_recv = swap(cov_send, 0, 2 * step)
        send, = call(sum_kernel, [units(g, BF16)], (send, recv))
        recv = swap(send, 0, step)
        cov_send, cov = call(
            bind(cov_second_kernel), [units(c, BF16), units(c, F32)],
            (cov, cov_recv))
        cov_recv = swap(cov_send, 0, step)
        cov, = call(sum_kernel, [units(c, BF16)], (cov, cov_recv))
        p_parts, q_parts = call(
            bind(inverses_kernel),
            [((2, plan.block, plan.block), BF16), ((2, 2, plan.block, plan.block), BF16)],
            (input_inverse.T, output_inverse.T, keep))
        done, = call(
            bind(finish_kernel), [units(2 * g, BF16)], (send, recv, p_parts, q_parts),
            scratch=[pltpu.VMEM(units(g, F32, 2)[0], F32)])
        y_done = swap(done, 0, 1)
        x_done = swap(done, 2, 0)
        d_done = swap(done, 2, 1)
        covs, = call(
            bind(join_kernel), [units(c, BF16, 4)],
            [cov, swap(cov, 0, 1), swap(cov, 2, 0),
             swap(cov, 2, 1)])
        in_factor, out_factor = call(
            bind(factors_kernel), [((plan.block, plan.owned), F32)] * 2,
            (covs, swap(covs, 1, 0)))
        result = [((width, width), BF16)]
        staging = [pltpu.VMEM((plan.block, width), BF16), pltpu.SemaphoreType.DMA]
        grad, = call(
            bind(early_kernel), result,
            (done, y_done, swap(done, 1, 0),
             swap(y_done, 1, 0)),
            hbm_out=1, scratch=staging * 2)
        x_away = swap(x_done, 1, 0)
        d_away = swap(d_done, 1, 0)
        grad, = call(
            group(lambda refs, outs: late_kernel(plan, 0, *refs, *outs), 3), result,
            (grad, x_done, d_done),
            hbm_in=1, hbm_out=1, aliases={0: 0}, scratch=staging)
        grad, = call(
            group(lambda refs, outs: late_kernel(plan, 1, *refs, *outs), 3), result,
            (grad, x_away, d_away),
            hbm_in=1, hbm_out=1, aliases={0: 0}, scratch=staging)
        return in_factor.T, out_factor.T, grad

    return jax.shard_map(
        shards,
        mesh=mesh,
        in_specs=(P(AXES, None), P(AXES, None), P(), P()),
        out_specs=(P("seq", None), P("seq", None), P()),
        check_vma=False,
    )
```
